128 devices in a mesh: row: 16 (over z, x), col: 8 (over y, core).
Axes of the slice: x: 4, y: 4, z: 4, core: 2. Of those that a mesh axis runs over, the one named last changes fastest.
Arguments:
- pole_values: float32 [65536], P('row'), may hold values from -32768 to 32768, as said below
- weights: float32 [65536], P('row'), may hold values from 0.15 to 0.5
- centers: float32 [65536], P('col'), as said below
- offsets: float32 [65536], P('col'), may hold values from -0.1 to 0.1
- chosen: int32 [2048], replicated, may hold values from 0 to 65535
- column_pole: int32 [2, 32768], P(None, 'row'), may hold values from 0 to 65535, as said below
- eigen_blocks: bfloat16 [6144, 2, 32768], P('col', None, 'row'), may hold values from -6 to 6
Outputs:
- roots_offset: float32 [65536], P('col')
- panel: float32 [6144, 2, 2048], P(('col', 'row'))
The draws below stay inside these ranges and needn't reach their ends.
Inputs may be any that keep to these rules, and one draw needn't show every extreme that they name: `pole_values`: ascending; consecutive poles differ by 1/4 to 7/4; every pole is a multiple of 1/128. centers[i] is the midpoint of pole_values[i] and pole_values[i + 1]; the last one is the last pole plus 1/2. `chosen`: indices of roots. `column_pole`: each of 0 to 65535 stands once.
All inputs are finite; a program needn't handle non-finite values.
Results may differ from the reference program's by a relative error of at most 0.0021.
Values may be sent and summed in bfloat16 or wider, within the bound.
No kernel may reach another device: no remote copies, remote signals or barrier semaphores. Data moves between devices by JAX's collectives and lax.ppermute only.
A program may use at most 128 MiB of HBM per device.

```python
import math
import jax
import jax.numpy as jnp
from jax import lax

N = 65536
H = 32768
ITERS = 3
K = 2048
QROWS = 6144


def pole_layout(key):
    marks = jax.random.randint(jax.random.fold_in(key, 11), (N,), 16, 113)
    return (jnp.arange(N) - N // 2).astype(jnp.float32) + marks.astype(jnp.float32) / 128.0


def draw_pole_values(key, part):
    return pole_layout(key)


def draw_centers(key, part):
    values = pole_layout(key)
    return jnp.concatenate([0.5 * (values[:-1] + values[1:]), values[-1:] + 0.5])


def draw_column_pole(key, part):
    return jax.random.permutation(jax.random.fold_in(key, 5), N).astype(jnp.int32).reshape(2, H)


def plant(drawn, stream_key, smallest, high):
    shape = drawn.shape
    place = [jax.random.randint(jax.random.fold_in(stream_key, axis), (), 0, shape[axis]) for axis in range(len(shape))]
    drawn = drawn.at[tuple(place)].set(smallest)
    longest = shape.index(max(shape))
    place[longest] = (place[longest] + 1) % shape[longest]
    return drawn.at[tuple(place)].set(high)


def steps_of(own_key, shape, shards, smallest, top_value):
    factor_of = 1.0
    for dim, shards_of in shards:
        heights = jax.random.uniform(jax.random.fold_in(jax.random.fold_in(own_key, 6), dim), (shards_of,), jnp.float32, smallest / len(shards), top_value / len(shards))
        factor_of = factor_of * jnp.repeat(jnp.exp(heights), shape[dim] // shards_of).reshape((-1,) + (1,) * (len(shape) - 1 - dim))
    return factor_of


def gaussian(key, dims, scale, most, split=(), dtype=jnp.bfloat16):
    entries = jax.random.normal(key, dims, jnp.float32) * scale
    if len(split) > 0:
        entries = steps_of(key, dims, split, -0.22, 0.18) * entries
    return jnp.clip(entries, min=-most, max=most).astype(dtype)


def setup_inputs(seed: int = 0) -> dict:
    key_of = jax.random.split(jax.random.key(seed), 8)
    pole_values = draw_pole_values(jax.random.fold_in(key_of[7], 71), 0)
    weights = jnp.clip(jnp.exp(math.log(0.5) - 1.2039728 * jax.random.uniform(key_of[1], (N,), jnp.float32) ** steps_of(key_of[1], (N,), ((0, 16),), -0.2, 0.2)), 0.15, 0.5)
    centers = draw_centers(jax.random.fold_in(key_of[7], 71), 0)
    offsets = jnp.clip(jax.random.uniform(key_of[3], (N,), jnp.float32, -0.1, 0.1) * steps_of(key_of[3], (N,), ((0, 8),), -0.4, 0.0), -0.1, 0.1)
    chosen = plant(jax.random.randint(key_of[4], (K,), 0, N), jax.random.fold_in(key_of[4], 1), 0, N - 1).astype(jnp.int32)
    column_pole = draw_column_pole(jax.random.fold_in(key_of[7], 71), 0)
    eigen_blocks = gaussian(key_of[6], (QROWS, 2, H), 1.0, 6.0, ((0, 8), (2, 16)))
    return {"pole_values": pole_values, "weights": weights, "centers": centers, "offsets": offsets, "chosen": chosen, "column_pole": column_pole, "eigen_blocks": eigen_blocks}


def block_sums(pole_vals, weight_sq, center_vals, offset_vals, block_rows):
    root_count = center_vals.shape[0]
    block_rows = min(block_rows, root_count)
    center_blocks = center_vals.reshape(root_count // block_rows, block_rows)
    offset_blocks = offset_vals.reshape(root_count // block_rows, block_rows)

    def per_block(blocks):
        distance = pole_vals[None, :] - blocks[0][:, None] - blocks[1][:, None]
        inverse = 1.0 / distance
        weighted = weight_sq[None, :] * inverse
        return (lax.optimization_barrier(jnp.sum(weighted, axis=1)), lax.optimization_barrier(jnp.sum(weighted * inverse, axis=1)), lax.optimization_barrier(jnp.min(jnp.abs(distance), axis=1)))
    sums = lax.map(per_block, (center_blocks, offset_blocks))
    return tuple((item.reshape(root_count) for item in sums))

def newton_update(offset_now, sum_inverse, sum_square, nearest):
    limit = 0.5 * nearest
    return offset_now - jnp.clip((1.0 + sum_inverse) / sum_square, -limit, limit)

def cauchy_block(pole_picked, weight_picked, panel_center, panel_offset, inv_norm):
    distance = pole_picked[:, None] - panel_center[None, :] - panel_offset[None, :]
    return (weight_picked[:, None] * (1.0 / distance) * inv_norm[None, :]).astype(jnp.bfloat16)

def reference(pole_values, weights, centers, offsets, chosen, column_pole, eigen_blocks):
    weight_sq = weights * weights
    offset_now = offsets
    for iteration in range(ITERS):
        sum_inverse, sum_square, nearest = block_sums(pole_values, weight_sq, centers, offset_now, 128)
        offset_now = newton_update(offset_now, sum_inverse, sum_square, nearest)
    panel_center = centers[chosen]
    panel_offset = offset_now[chosen]
    norm_sq = block_sums(pole_values, weight_sq, panel_center, panel_offset, 64)[1]
    inv_norm = lax.rsqrt(norm_sq)
    halves_out = []
    for half_index in range(2):
        pole_index = column_pole[half_index]
        cauchy = cauchy_block(pole_values[pole_index], weights[pole_index], panel_center, panel_offset, inv_norm)
        halves_out.append(jnp.dot(eigen_blocks[:, half_index, :], cauchy, preferred_element_type=jnp.float32))
    return (offset_now, jnp.stack(halves_out, axis=1))
```

```python
import jax
import jax.numpy as jnp
from jax import lax
from jax.experimental import pallas as pl
from jax.experimental.pallas import tpu as pltpu
from jax.sharding import Mesh
from jax.sharding import PartitionSpec as P

ITERS = 3
ROW = ("z", "x")
COL = ("y", "core")
ALL = ("z", "x", "y", "core")
F32 = jnp.float32
BF16 = jnp.bfloat16
LANES = 128
GROUP = 64
UNROLL = 32
SPLIT = 3


def cost(flops):
    return pl.CostEstimate(flops=int(flops), bytes_accessed=1 << 20, transcendentals=0)


def column(row):
    return jnp.broadcast_to(row, (LANES, LANES)).T


def load_tables(pw_ref, w2_ref):
    parts, _, rows, _ = pw_ref.shape
    for part in range(parts):
        w = pw_ref[part, 1]
        w2_ref[part * rows : (part + 1) * rows, :] = w * w


def shift_poles(pw_ref, ps_ref, base):
    parts, _, rows, _ = pw_ref.shape
    for part in range(parts):
        ps_ref[part * rows : (part + 1) * rows, :] = pw_ref[part, 0] - base


def root_kernel(pw_ref, root_ref, out_ref, w2_ref, ps_ref, c_ref, t_ref, lo_ref, hi_ref):
    load_tables(pw_ref, w2_ref)
    n_rows = root_ref.shape[1]
    for k in range(n_rows):
        here = pl.ds(k * LANES, LANES)
        c_ref[here, :] = column(root_ref[0, k : k + 1, :])
        t_ref[here, :] = column(root_ref[1, k : k + 1, :])
        lo_ref[here, :] = column(root_ref[2, k : k + 1, :])
        hi_ref[here, :] = column(root_ref[3, k : k + 1, :])

    def group_body(g, carry):
        here = pl.ds(g * GROUP, GROUP)
        c = c_ref[here, :]
        base = c_ref[pl.ds(g * GROUP + GROUP // 2, 1), :]
        shift_poles(pw_ref, ps_ref, base)
        near = c - base

        def step(_, carry):
            t = t_ref[here, :]
            s = near + t

            def body(r, sums):
                first, second = sums
                for u in range(UNROLL):
                    row = pl.ds(r * UNROLL + u, 1)
                    inverse = 1.0 / (ps_ref[row, :] - s)
                    weighted = w2_ref[row, :] * inverse
                    first = first + weighted
                    second = second + weighted * inverse
                return first, second

            zero = jnp.zeros((GROUP, LANES), F32)
            first, second = lax.fori_loop(0, ps_ref.shape[0] // UNROLL, body, (zero, zero))
            sum_inverse = jnp.sum(first, axis=1, keepdims=True)
            sum_square = jnp.sum(second, axis=1, keepdims=True)
            nearest = jnp.minimum(jnp.abs(lo_ref[here, :] - t), jnp.abs(hi_ref[here, :] - t))
            limit = 0.5 * nearest
            t_ref[here, :] = t - jnp.clip((1.0 + sum_inverse) / sum_square, -limit, limit)
            return carry

        lax.fori_loop(0, ITERS, step, 0)
        return carry

    lax.fori_loop(0, n_rows * LANES // GROUP, group_body, 0)
    for k in range(n_rows):
        out_ref[k : k + 1, :] = t_ref[pl.ds(k * LANES, LANES), :].T[0:1, :]


def find_roots(pw, root):
    n_rows = root.shape[1]
    n_pole_rows = pw.shape[0] * pw.shape[2]
    roots = n_rows * LANES
    return pl.pallas_call(
        root_kernel,
        out_shape=jax.ShapeDtypeStruct((n_rows, LANES), F32),
        scratch_shapes=[pltpu.VMEM((n_pole_rows, LANES), F32)] * 2
        + [pltpu.VMEM((roots, LANES), F32)] * 4,
        cost_estimate=cost(ITERS * roots * n_pole_rows * LANES * 10),
        name="find_roots",
    )(pw, root)


def panel_kernel(pw_ref, root_ref, out_ref, w2_ref):
    load_tables(pw_ref, w2_ref)
    parts, _, rows, _ = pw_ref.shape
    count = 16
    c = column(root_ref[0:1, :])[:count]
    t = column(root_ref[1:2, :])[:count]
    unroll = 16
    per_part = rows // unroll

    def sums_at(t):
        def body(r, sums):
            first, second, nearest = sums
            part = r // per_part
            start = (r % per_part) * unroll
            for u in range(unroll):
                distance = (pw_ref[part, 0, pl.ds(start + u, 1), :] - c) - t
                inverse = 1.0 / distance
                weighted = w2_ref[pl.ds(r * unroll + u, 1), :] * inverse
                first = first + weighted
                second = second + weighted * inverse
                nearest = jnp.minimum(nearest, jnp.abs(distance))
            return first, second, nearest

        zero = jnp.zeros((count, LANES), F32)
        first, second, nearest = lax.fori_loop(
            0, parts * per_part, body, (zero, zero, jnp.full((count, LANES), 3e38, F32))
        )
        return (
            jnp.sum(first, axis=1, keepdims=True),
            jnp.sum(second, axis=1, keepdims=True),
            jnp.min(nearest, axis=1, keepdims=True),
        )

    for _ in range(ITERS):
        sum_inverse, sum_square, nearest = sums_at(t)
        limit = 0.5 * nearest
        t = t - jnp.clip((1.0 + sum_inverse) / sum_square, -limit, limit)
    norm = lax.rsqrt(sums_at(t)[1])
    pad = jnp.zeros((LANES - count, LANES), F32)
    out_ref[0:1, :] = jnp.concatenate([t, pad], axis=0).T[0:1, :]
    out_ref[1:2, :] = jnp.concatenate([jnp.broadcast_to(norm, (count, LANES)), pad], axis=0).T[0:1, :]


def panel_roots(pw, root):
    n_pole_rows = pw.shape[0] * pw.shape[2]
    return pl.pallas_call(
        panel_kernel,
        out_shape=jax.ShapeDtypeStruct((2, LANES), F32),
        scratch_shapes=[pltpu.VMEM((n_pole_rows, LANES), F32)],
        cost_estimate=cost(4 * 20 * n_pole_rows * LANES * 10),
        name="panel_roots",
    )(pw, root)


def pick_kernel(index_ref, pw_ref, out_ref):
    parts, _, rows, _ = pw_ref.shape
    index = jnp.concatenate([index_ref[...], index_ref[...]], axis=0)
    row = index // LANES
    lane = index % LANES
    unroll = 16
    per_part = rows // unroll

    def body(r, carry):
        p, w = carry
        part = r // per_part
        start = (r % per_part) * unroll
        for u in range(unroll):
            hit = row == r * unroll + u
            p_row = jnp.broadcast_to(pw_ref[part, 0, pl.ds(start + u, 1), :], (8, LANES))
            w_row = jnp.broadcast_to(pw_ref[part, 1, pl.ds(start + u, 1), :], (8, LANES))
            p = jnp.where(hit, jnp.take_along_axis(p_row, lane, axis=1), p)
            w = jnp.where(hit, jnp.take_along_axis(w_row, lane, axis=1), w)
        return p, w

    zero = jnp.zeros((8, LANES), F32)
    p, w = lax.fori_loop(0, parts * per_part, body, (zero, zero))
    out_ref[0] = p[:4]
    out_ref[1] = w[:4]


def pick_columns(index, pw):
    return pl.pallas_call(
        pick_kernel,
        out_shape=jax.ShapeDtypeStruct((2, 4, LANES), F32),
        cost_estimate=cost(5e7),
        name="pick_columns",
    )(index, pw)


def matmul_kernel(
    col_ref, root_ref, e0, e1, e2, e3, own_ref, send_ref, p_ref, w_ref, tile_a, tile_b, acc_ref
):
    blocks = (e0, e1, e2, e3)
    halves, rows, depth = e0.shape
    chunk = tile_a.shape[1]
    chunks = root_ref.shape[1] // chunk
    pieces = depth // LANES
    for piece in range(p_ref.shape[0] // LANES):
        here = pl.ds(piece * LANES, LANES)
        p_ref[here, :] = column(col_ref[0, piece : piece + 1, :])
        w_ref[here, :] = column(col_ref[1, piece : piece + 1, :])

    def fill(tile, src, half, k):
        for part in range(chunk // LANES):
            lanes = pl.ds(k * chunk + part * LANES, LANES)
            c = root_ref[0:1, lanes]
            t = root_ref[1:2, lanes]
            n = root_ref[2:3, lanes]
            for piece in range(pieces):
                here = pl.ds((src * halves + half) * depth + piece * LANES, LANES)
                distance = (p_ref[here, :] - c) - t
                value = w_ref[here, :] * (1.0 / distance) * n
                tile[piece * LANES : (piece + 1) * LANES, part * LANES : (part + 1) * LANES] = (
                    value.astype(BF16)
                )

    def product(src, half, tile):
        return jnp.dot(blocks[src][half], tile[...], preferred_element_type=F32)

    steps = halves * chunks
    fill(tile_a, 0, 0, 0)

    def body(i, carry):
        half = i // chunks
        k = i % chunks
        following = jnp.minimum(i + 1, steps - 1)
        fill(tile_b, 1, half, k)
        acc_ref[...] = product(0, half, tile_a)
        fill(tile_a, 2, half, k)
        acc_ref[...] += product(1, half, tile_b)
        fill(tile_b, 3, half, k)
        acc_ref[...] += product(2, half, tile_a)
        fill(tile_a, 0, following // chunks, following % chunks)
        acc = acc_ref[...] + product(3, half, tile_b)
        quarter = rows // 4
        for part in range(4):
            piece = acc[part * quarter : (part + 1) * quarter]
            own_ref[part, half, :, pl.ds(k * chunk, chunk)] = piece
            send_ref[part, half, :, pl.ds(k * chunk, chunk)] = piece.astype(BF16)
        return carry

    lax.fori_loop(0, steps, body, 0)


def panel_product(columns, root, blocks):
    halves, rows, depth = blocks[0].shape
    n_roots = root.shape[1]
    chunk = 256
    shape = (4, halves, rows // 4, n_roots)
    return pl.pallas_call(
        matmul_kernel,
        out_shape=(jax.ShapeDtypeStruct(shape, F32), jax.ShapeDtypeStruct(shape, BF16)),
        scratch_shapes=[pltpu.VMEM((4 * halves * depth, LANES), F32)] * 2
        + [pltpu.VMEM((depth, chunk), BF16)] * 2
        + [pltpu.VMEM((rows, chunk), F32)],
        cost_estimate=cost(2 * 4 * halves * rows * depth * n_roots),
        name="panel_product",
    )(columns, root, *blocks)


def copies(value, axis):
    size = lax.axis_size(axis)
    return lax.all_to_all(
        jnp.broadcast_to(value[None], (size, *value.shape)), axis, 0, 0, tiled=True
    )


def ring(shift):
    return [(i, (i + shift) % 4) for i in range(4)]


def on_device(pole_values, weights, centers, offsets, chosen, column_pole, eigen_blocks):
    z = lax.axis_index("z")
    x = lax.axis_index("x")
    row = z * 4 + x
    col = lax.axis_index("y") * 2 + lax.axis_index("core")
    n_col = centers.shape[0]
    n_own = n_col // 16

    parted = jnp.stack([pole_values.reshape(-1, LANES), weights.reshape(-1, LANES)])
    pw = copies(parted, ROW)

    turned = jnp.moveaxis(eigen_blocks.reshape(4, -1, 2, eigen_blocks.shape[2]), 2, 1)
    blocks = [lax.dynamic_index_in_dim(turned, z, 0, keepdims=False)]
    for shift in (1, 2, 3):
        block = lax.dynamic_index_in_dim(turned, (z + shift) % 4, 0, keepdims=False)
        blocks.append(lax.ppermute(block, "z", ring(shift)))

    wanted = lax.dynamic_slice_in_dim(chosen, row * LANES, LANES)
    local = wanted - col * n_col
    hit = local[:, None] == lax.broadcasted_iota(jnp.int32, (1, n_col), 1)
    first = jnp.stack(
        [
            jnp.sum(jnp.where(hit, centers[None, :], 0.0), axis=1),
            jnp.sum(jnp.where(hit, offsets[None, :], 0.0), axis=1),
        ]
    )
    spread = jnp.moveaxis(first.reshape(2, 8, 16), 1, 0)
    mine = jnp.sum(lax.all_to_all(spread, COL, 0, 0, tiled=True), axis=0)
    panel_start = jnp.pad(mine, ((0, 0), (0, LANES - 16)), constant_values=0.25)
    panel_end = panel_roots(pw, panel_start)

    index = lax.dynamic_slice_in_dim(column_pole.reshape(-1, LANES), col * 4, 4)
    picked = pick_columns(index, pw)

    note = jnp.concatenate([picked.reshape(8, LANES), panel_start[:1], panel_end], axis=0)
    notes = copies(note, ALL)
    columns = lax.dynamic_index_in_dim(
        notes[:, :8].reshape(4, 4, 8, 2, 4, LANES), x, 1, keepdims=False
    )
    columns = jnp.concatenate(
        [lax.dynamic_slice_in_dim(jnp.concatenate([columns, columns]), (z - s) % 4, 1) for s in range(4)]
    )
    columns = jnp.moveaxis(columns, 2, 0).reshape(2, -1, LANES)
    panel_root = jnp.moveaxis(notes[:, 8:, :16], 1, 0).reshape(3, -1)

    start = col * n_col + row * n_own
    my_centers = lax.dynamic_slice_in_dim(centers, row * n_own, n_own)
    my_offsets = lax.dynamic_slice_in_dim(offsets, row * n_own, n_own)
    part = start // pole_values.shape[0]
    own_poles = lax.dynamic_slice(
        pw.reshape(16, 2, -1), (part, 0, start - part * pole_values.shape[0]), (1, 1, n_own)
    ).reshape(n_own)
    low = own_poles - my_centers
    last = start + jnp.arange(n_own) == pole_values.shape[0] * 16 - 1
    high = jnp.where(last, 3e38, -low)
    mine = jnp.stack([my_centers, my_offsets, low, high]).reshape(4, -1, LANES)
    roots_a = find_roots(pw, mine[:, :SPLIT])

    own, send = panel_product(columns, panel_root, blocks)
    pieces = [lax.dynamic_index_in_dim(own, x, 0, keepdims=False)]
    for shift in (1, 2, 3):
        piece = lax.dynamic_index_in_dim(send, (x + shift) % 4, 0, keepdims=False)
        pieces.append(lax.ppermute(piece, "x", ring(shift)))

    roots_b = find_roots(pw, mine[:, SPLIT:])
    panel = pieces[0] + pieces[1] + pieces[2] + pieces[3]
    panel = jnp.moveaxis(panel, 0, 1)
    roots = copies(jnp.concatenate([roots_a, roots_b]), ROW)
    return roots.reshape(-1), panel


def solution(mesh):
    torus = Mesh(mesh.devices.reshape(4, 4, 4, 2), ALL)
    placed = (P(ROW), P(ROW), P(COL), P(COL), P(), P(None, ROW), P(COL, None, ROW))
    return jax.shard_map(
        on_device,
        mesh=torus,
        in_specs=placed,
        out_specs=(P(COL), P(COL + ROW, None, None)),
        check_vma=False,
    )
```

```python
import jax
import jax.numpy as jnp
from jax import lax
from jax.experimental import pallas as pl
from jax.experimental.pallas import tpu as pltpu
from jax.sharding import Mesh
from jax.sharding import PartitionSpec as P

ITERS = 3
ROW = ("z", "x")
COL = ("y", "core")
ALL = ("z", "x", "y", "core")
F32 = jnp.float32
BF16 = jnp.bfloat16
LANES = 128
GROUP = 64
UNROLL = 32
CUT_A = 5
CUT_B = 6


def cost(flops):
    return pl.CostEstimate(flops=int(flops), bytes_accessed=1 << 20, transcendentals=0)


def column(row):
    return jnp.broadcast_to(row, (LANES, LANES)).T


def load_tables(pw_ref, w2_ref):
    parts, _, rows, _ = pw_ref.shape
    for part in range(parts):
        w = pw_ref[part, 1]
        w2_ref[part * rows : (part + 1) * rows, :] = w * w


def shift_poles(pw_ref, ps_ref, base):
    parts, _, rows, _ = pw_ref.shape
    for part in range(parts):
        ps_ref[part * rows : (part + 1) * rows, :] = pw_ref[part, 0] - base


def root_kernel(pw_ref, root_ref, out_ref, w2_ref, ps_ref, c_ref, t_ref, lo_ref, hi_ref):
    load_tables(pw_ref, w2_ref)
    groups = root_ref.shape[1]
    for k in range(groups):
        here = pl.ds(k * GROUP, GROUP)
        c_ref[here, :] = column(root_ref[0, k : k + 1, :])[:GROUP]
        t_ref[here, :] = column(root_ref[1, k : k + 1, :])[:GROUP]
        lo_ref[here, :] = column(root_ref[2, k : k + 1, :])[:GROUP]
        hi_ref[here, :] = column(root_ref[3, k : k + 1, :])[:GROUP]

    def group_body(g, carry):
        here = pl.ds(g * GROUP, GROUP)
        base = c_ref[pl.ds(g * GROUP + GROUP // 2, 1), :]
        shift_poles(pw_ref, ps_ref, base)
        near = c_ref[here, :] - base

        def step(_, carry):
            t = t_ref[here, :]
            s = near + t

            def body(r, sums):
                first, second = sums
                for u in range(UNROLL):
                    row = pl.ds(r * UNROLL + u, 1)
                    inverse = 1.0 / (ps_ref[row, :] - s)
                    weighted = w2_ref[row, :] * inverse
                    first = first + weighted
                    second = second + weighted * inverse
                return first, second

            zero = jnp.zeros((GROUP, LANES), F32)
            first, second = lax.fori_loop(0, ps_ref.shape[0] // UNROLL, body, (zero, zero))
            sum_inverse = jnp.sum(first, axis=1, keepdims=True)
            sum_square = jnp.sum(second, axis=1, keepdims=True)
            nearest = jnp.minimum(jnp.abs(lo_ref[here, :] - t), jnp.abs(hi_ref[here, :] - t))
            limit = 0.5 * nearest
            t_ref[here, :] = t - jnp.clip((1.0 + sum_inverse) / sum_square, -limit, limit)
            return carry

        lax.fori_loop(0, ITERS, step, 0)
        return carry

    lax.fori_loop(0, groups, group_body, 0)
    pad = jnp.zeros((LANES - GROUP, LANES), F32)
    for k in range(groups):
        t = jnp.concatenate([t_ref[pl.ds(k * GROUP, GROUP), :], pad], axis=0)
        out_ref[k : k + 1, :] = t.T[0:1, :]


def find_roots(pw, root):
    groups = root.shape[1]
    n_pole_rows = pw.shape[0] * pw.shape[2]
    roots = groups * GROUP
    root = jnp.pad(root, ((0, 0), (0, 0), (0, LANES - GROUP)))
    found = pl.pallas_call(
        root_kernel,
        out_shape=jax.ShapeDtypeStruct((groups, LANES), F32),
        scratch_shapes=[pltpu.VMEM((n_pole_rows, LANES), F32)] * 2
        + [pltpu.VMEM((roots, LANES), F32)] * 4,
        cost_estimate=cost(ITERS * roots * n_pole_rows * LANES * 10),
        name="find_roots",
    )(pw, root)
    return found[:, :GROUP]


def panel_kernel(pw_ref, root_ref, out_ref, w2_ref):
    load_tables(pw_ref, w2_ref)
    parts, _, rows, _ = pw_ref.shape
    count = 16
    c = column(root_ref[0:1, :])[:count]
    t = column(root_ref[1:2, :])[:count]
    unroll = 16
    per_part = rows // unroll

    def sums_at(t):
        def body(r, sums):
            first, second, nearest = sums
            part = r // per_part
            start = (r % per_part) * unroll
            for u in range(unroll):
                distance = (pw_ref[part, 0, pl.ds(start + u, 1), :] - c) - t
                inverse = 1.0 / distance
                weighted = w2_ref[pl.ds(r * unroll + u, 1), :] * inverse
                first = first + weighted
                second = second + weighted * inverse
                nearest = jnp.minimum(nearest, jnp.abs(distance))
            return first, second, nearest

        zero = jnp.zeros((count, LANES), F32)
        first, second, nearest = lax.fori_loop(
            0, parts * per_part, body, (zero, zero, jnp.full((count, LANES), 3e38, F32))
        )
        return (
            jnp.sum(first, axis=1, keepdims=True),
            jnp.sum(second, axis=1, keepdims=True),
            jnp.min(nearest, axis=1, keepdims=True),
        )

    for _ in range(ITERS):
        sum_inverse, sum_square, nearest = sums_at(t)
        limit = 0.5 * nearest
        t = t - jnp.clip((1.0 + sum_inverse) / sum_square, -limit, limit)
    norm = lax.rsqrt(sums_at(t)[1])
    pad = jnp.zeros((LANES - count, LANES), F32)
    out_ref[0:1, :] = jnp.concatenate([t, pad], axis=0).T[0:1, :]
    out_ref[1:2, :] = jnp.concatenate([jnp.broadcast_to(norm, (count, LANES)), pad], axis=0).T[0:1, :]


def panel_roots(pw, root):
    n_pole_rows = pw.shape[0] * pw.shape[2]
    return pl.pallas_call(
        panel_kernel,
        out_shape=jax.ShapeDtypeStruct((2, LANES), F32),
        scratch_shapes=[pltpu.VMEM((n_pole_rows, LANES), F32)],
        cost_estimate=cost(4 * 20 * n_pole_rows * LANES * 10),
        name="panel_roots",
    )(pw, root)


def pick_kernel(index_ref, pw_ref, out_ref):
    parts, _, rows, _ = pw_ref.shape
    index = jnp.concatenate([index_ref[...], index_ref[...]], axis=0)
    row = index // LANES
    lane = index % LANES
    unroll = 16
    per_part = rows // unroll

    def body(r, carry):
        p, w = carry
        part = r // per_part
        start = (r % per_part) * unroll
        for u in range(unroll):
            hit = row == r * unroll + u
            p_row = jnp.broadcast_to(pw_ref[part, 0, pl.ds(start + u, 1), :], (8, LANES))
            w_row = jnp.broadcast_to(pw_ref[part, 1, pl.ds(start + u, 1), :], (8, LANES))
            p = jnp.where(hit, jnp.take_along_axis(p_row, lane, axis=1), p)
            w = jnp.where(hit, jnp.take_along_axis(w_row, lane, axis=1), w)
        return p, w

    zero = jnp.zeros((8, LANES), F32)
    p, w = lax.fori_loop(0, parts * per_part, body, (zero, zero))
    out_ref[0] = p[:4]
    out_ref[1] = w[:4]


def pick_columns(index, pw):
    return pl.pallas_call(
        pick_kernel,
        out_shape=jax.ShapeDtypeStruct((2, 4, LANES), F32),
        cost_estimate=cost(5e7),
        name="pick_columns",
    )(index, pw)


def matmul_kernel(col_ref, root_ref, *refs):
    blocks = refs[:8]
    own_ref, send_ref, p_ref, w_ref = refs[8:]
    sources = 4
    _, rows, depth = blocks[0].shape
    chunk = 256
    chunks = root_ref.shape[1] // chunk
    pieces = depth // LANES
    for src in range(sources):
        p = jnp.concatenate([col_ref[0, src, 0]] * (LANES // pieces), axis=0).T
        w = jnp.concatenate([col_ref[1, src, 0]] * (LANES // pieces), axis=0).T
        for piece in range(pieces):
            here = pl.ds(src * depth + piece * LANES, LANES)
            p_ref[here, :] = jnp.broadcast_to(p[:, piece : piece + 1], (LANES, LANES))
            w_ref[here, :] = jnp.broadcast_to(w[:, piece : piece + 1], (LANES, LANES))

    def cauchy(src, k):
        down = []
        for piece in range(pieces):
            here = pl.ds(src * depth + piece * LANES, LANES)
            p = p_ref[here, :]
            w = w_ref[here, :]
            across = []
            for part in range(chunk // LANES):
                lanes = pl.ds(k * chunk + part * LANES, LANES)
                distance = (p - root_ref[0:1, lanes]) - root_ref[1:2, lanes]
                value = w * (1.0 / distance) * root_ref[2:3, lanes]
                across.append(value.astype(BF16))
            down.append(jnp.concatenate(across, axis=1))
        return jnp.concatenate(down, axis=0)

    def body(k, carry):
        acc = None
        for src in range(sources):
            left = jnp.concatenate([blocks[src][0], blocks[sources + src][0]], axis=0)
            product = jnp.dot(left, cauchy(src, k), preferred_element_type=F32)
            acc = product if acc is None else acc + product
        quarter = rows // 4
        for part in range(4):
            for side in range(2):
                first = side * rows + part * quarter
                piece = acc[first : first + quarter]
                own_ref[part, 0, side, :, pl.ds(k * chunk, chunk)] = piece
                send_ref[part, 0, side, :, pl.ds(k * chunk, chunk)] = piece.astype(BF16)
        return carry

    lax.fori_loop(0, chunks, body, 0)


def panel_product(columns, root, blocks):
    sources = 4
    halves, rows, depth = blocks[0].shape
    n_roots = root.shape[1]
    pieces = depth // LANES
    shape = (4, halves, 2, rows // 4, n_roots)
    out = pl.BlockSpec((4, 1, 2, rows // 4, n_roots), lambda h: (0, h, 0, 0, 0))
    block = pl.BlockSpec((1, rows, depth), lambda h: (h, 0, 0))
    return pl.pallas_call(
        matmul_kernel,
        grid=(halves,),
        in_specs=[
            pl.BlockSpec((2, sources, 1, pieces, LANES), lambda h: (0, 0, h, 0, 0)),
            pl.BlockSpec((3, n_roots), lambda h: (0, 0)),
        ]
        + [block] * 8,
        out_specs=(out, out),
        out_shape=(jax.ShapeDtypeStruct(shape, F32), jax.ShapeDtypeStruct(shape, BF16)),
        scratch_shapes=[pltpu.VMEM((sources * depth, LANES), F32)] * 2,
        compiler_params=pltpu.CompilerParams(vmem_limit_bytes=56 << 20),
        cost_estimate=cost(2 * 2 * sources * halves * rows * depth * n_roots),
        name="panel_product",
    )(columns.reshape(2, sources, halves, pieces, LANES), root, *blocks)


def copies(value, axis):
    size = lax.axis_size(axis)
    return lax.all_to_all(
        jnp.broadcast_to(value[None], (size, *value.shape)), axis, 0, 0, tiled=True
    )


def ring(shift):
    return [(i, (i + shift) % 4) for i in range(4)]


def merge(pole_values, weights, centers, offsets, chosen, column_pole, eigen_blocks):
    z = lax.axis_index("z")
    x = lax.axis_index("x")
    core = lax.axis_index("core")
    row = z * 4 + x
    col = lax.axis_index("y") * 2 + core
    n_col = centers.shape[0]
    n_own = n_col // 16
    swap = [(0, 1), (1, 0)]

    parted = jnp.stack([pole_values.reshape(-1, LANES), weights.reshape(-1, LANES)])
    pw = copies(parted, ROW)

    turned = jnp.moveaxis(eigen_blocks.reshape(4, -1, 2, eigen_blocks.shape[2]), 2, 1)

    wanted = lax.dynamic_slice_in_dim(chosen, row * LANES, LANES)
    local = wanted - col * n_col
    hit = local[:, None] == lax.broadcasted_iota(jnp.int32, (1, n_col), 1)
    first = jnp.stack(
        [
            jnp.sum(jnp.where(hit, centers[None, :], 0.0), axis=1),
            jnp.sum(jnp.where(hit, offsets[None, :], 0.0), axis=1),
        ]
    )
    spread = jnp.moveaxis(first.reshape(2, 8, 16), 1, 0)
    arrived = lax.all_to_all(spread, COL, 0, 0, tiled=True)
    pw, turned, arrived = lax.optimization_barrier((pw, turned, arrived))
    eigen = [lax.dynamic_index_in_dim(turned, z, 0, keepdims=False)]
    for shift in (1, 2, 3):
        block = lax.dynamic_index_in_dim(turned, (z + shift) % 4, 0, keepdims=False)
        eigen.append(lax.ppermute(block, "z", ring(shift)))
    peer = [lax.ppermute(eigen[0], "core", swap)]

    panel_start = jnp.pad(
        jnp.sum(arrived, axis=0), ((0, 0), (0, LANES - 16)), constant_values=0.25
    )
    panel_end = panel_roots(pw, panel_start)
    index = lax.dynamic_slice_in_dim(column_pole.reshape(-1, LANES), col * 4, 4)
    picked = pick_columns(index, pw)
    note = jnp.concatenate([picked.reshape(8, LANES), panel_start[:1], panel_end], axis=0)
    notes = copies(note, ALL)

    start = col * n_col + row * n_own
    my_centers = lax.dynamic_slice_in_dim(centers, row * n_own, n_own)
    my_offsets = lax.dynamic_slice_in_dim(offsets, row * n_own, n_own)
    part = start // pole_values.shape[0]
    own_poles = lax.dynamic_slice(
        pw.reshape(16, 2, -1), (part, 0, start - part * pole_values.shape[0]), (1, 1, n_own)
    ).reshape(n_own)
    low = own_poles - my_centers
    last = start + jnp.arange(n_own) == pole_values.shape[0] * 16 - 1
    high = jnp.where(last, 3e38, -low)
    state = jnp.stack([my_centers, my_offsets, low, high]).reshape(4, -1, GROUP)
    roots_a = find_roots(pw, state[:, :CUT_A])
    eigen, notes, roots_a = lax.optimization_barrier((eigen, notes, roots_a))

    peer += [lax.ppermute(block, "core", swap) for block in eigen[1:]]
    roots_b = find_roots(pw, state[:, CUT_A:CUT_B])

    columns = lax.dynamic_index_in_dim(
        notes[:, :8].reshape(4, 4, 8, 2, 4, LANES), x, 1, keepdims=False
    )
    columns = jnp.concatenate(
        [lax.dynamic_slice_in_dim(columns, (z - s) % 4, 1) for s in range(4)]
    )
    columns = jnp.moveaxis(columns, 2, 0)
    panel_root = jnp.moveaxis(notes[:, 8:, :16], 1, 0).reshape(3, 2, -1)
    panel_root = lax.dynamic_index_in_dim(panel_root, core, 1, keepdims=False)
    panel_root, peer, roots_b = lax.optimization_barrier((panel_root, peer, roots_b))
    own, send = panel_product(columns, panel_root, eigen + peer)

    pieces = [lax.dynamic_index_in_dim(own, x, 0, keepdims=False)]
    for shift in (1, 2, 3):
        piece = lax.dynamic_index_in_dim(send, (x + shift) % 4, 0, keepdims=False)
        pieces.append(lax.ppermute(piece, "x", ring(shift)))
    roots_c = find_roots(pw, state[:, CUT_B:])
    total = pieces[0] + pieces[1] + pieces[2] + pieces[3]
    keep = total[:, 0]
    got = lax.ppermute(total[:, 1], "core", swap)
    roots = copies(jnp.concatenate([roots_a, roots_b, roots_c]), ROW)
    panel = jnp.where(
        core == 0, jnp.concatenate([keep, got], axis=2), jnp.concatenate([got, keep], axis=2)
    )
    return roots.reshape(-1), jnp.moveaxis(panel, 0, 1)


def solution(mesh):
    torus = Mesh(mesh.devices.reshape(4, 4, 4, 2), ALL)
    placed = (P(ROW), P(ROW), P(COL), P(COL), P(), P(None, ROW), P(COL, None, ROW))
    return jax.shard_map(
        merge,
        mesh=torus,
        in_specs=placed,
        out_specs=(P(COL), P(COL + ROW, None, None)),
        check_vma=False,
    )
```

```python
import jax
import jax.numpy as jnp
from jax import lax
from jax.experimental import pallas as pl
from jax.experimental.pallas import tpu as pltpu
from jax.sharding import Mesh
from jax.sharding import PartitionSpec as P

ITERS = 3
ROW = ("z", "x")
COL = ("y", "core")
ALL = ("z", "x", "y", "core")
F32 = jnp.float32
BF16 = jnp.bfloat16
LANES = 128
GROUP = 128
BLOCK = 16
CUT_A = 2
CUT_B = 3


def cost(flops):
    return pl.CostEstimate(flops=int(flops), bytes_accessed=1 << 20, transcendentals=0)


def column(row):
    return jnp.broadcast_to(row, (LANES, LANES)).T


def load_tables(pw_ref, w2_ref):
    parts, _, rows, _ = pw_ref.shape
    for part in range(parts):
        w = pw_ref[part, 1]
        w2_ref[part * rows : (part + 1) * rows, :] = w * w


def shift_poles(pw_ref, ps_ref, base):
    parts, _, rows, _ = pw_ref.shape
    for part in range(parts):
        ps_ref[part * rows : (part + 1) * rows, :] = pw_ref[part, 0] - base


def root_kernel(rank_ref, pw_ref, root_ref, out_ref, w2_ref, ps_ref, c_ref, t_ref, lo_ref, hi_ref):
    load_tables(pw_ref, w2_ref)
    groups = root_ref.shape[1]
    blocks = ps_ref.shape[0] // BLOCK
    for k in range(groups):
        here = pl.ds(k * GROUP, GROUP)
        c_ref[here, :] = column(root_ref[0, k : k + 1, :])
        t_ref[here, :] = column(root_ref[1, k : k + 1, :])
        lo_ref[here, :] = column(root_ref[2, k : k + 1, :])
        hi_ref[here, :] = column(root_ref[3, k : k + 1, :])

    def group_body(g, carry):
        here = pl.ds(g * GROUP, GROUP)
        base = c_ref[pl.ds(g * GROUP + GROUP // 2, 1), :]
        shift_poles(pw_ref, ps_ref, base)
        offset = c_ref[here, :] - base
        near_block = jnp.clip((rank_ref[0] // LANES + g - BLOCK // 2) // BLOCK, 0, blocks - 2)

        def step(_, carry):
            t = t_ref[here, :]
            s = offset + t

            def near(r, sums):
                first, second = sums
                for u in range(BLOCK):
                    row = pl.ds((near_block + r) * BLOCK + u, 1)
                    inverse = 1.0 / (ps_ref[row, :] - s)
                    weighted = w2_ref[row, :] * inverse
                    first = first + weighted
                    second = second + weighted * inverse
                return first, second

            def far(i, sums):
                first, second = sums
                for half in range(2):
                    block = 2 * i + half
                    block = jnp.where(block >= near_block, block + 2, block)
                    some = None
                    for u in range(BLOCK):
                        row = pl.ds(block * BLOCK + u, 1)
                        distance = (ps_ref[row, :] - s).astype(BF16)
                        weight = jnp.broadcast_to(w2_ref[row, :], (GROUP, LANES)).astype(BF16)
                        weighted = weight / distance
                        square = weighted / distance
                        some = (weighted, square) if some is None else (some[0] + weighted, some[1] + square)
                    first = first + some[0].astype(F32)
                    second = second + some[1].astype(F32)
                return first, second

            zero = jnp.zeros((GROUP, LANES), F32)
            sums = lax.fori_loop(0, 2, near, (zero, zero))
            first, second = lax.fori_loop(0, (blocks - 2) // 2, far, sums)
            sum_inverse = jnp.sum(first, axis=1, keepdims=True)
            sum_square = jnp.sum(second, axis=1, keepdims=True)
            nearest = jnp.minimum(jnp.abs(lo_ref[here, :] - t), jnp.abs(hi_ref[here, :] - t))
            limit = 0.5 * nearest
            t_ref[here, :] = t - jnp.clip((1.0 + sum_inverse) / sum_square, -limit, limit)
            return carry

        lax.fori_loop(0, ITERS, step, 0)
        return carry

    lax.fori_loop(0, groups, group_body, 0)
    for k in range(groups):
        out_ref[k : k + 1, :] = t_ref[pl.ds(k * GROUP, GROUP), :].T[0:1, :]


def find_roots(rank, pw, root):
    groups = root.shape[1]
    n_pole_rows = pw.shape[0] * pw.shape[2]
    roots = groups * GROUP
    vmem = pl.BlockSpec(memory_space=pltpu.VMEM)
    return pl.pallas_call(
        root_kernel,
        in_specs=[pl.BlockSpec(memory_space=pltpu.SMEM), vmem, vmem],
        out_shape=jax.ShapeDtypeStruct((groups, LANES), F32),
        scratch_shapes=[pltpu.VMEM((n_pole_rows, LANES), F32)] * 2
        + [pltpu.VMEM((roots, LANES), F32)] * 4,
        cost_estimate=cost(ITERS * roots * n_pole_rows * LANES * 10),
        name="find_roots",
    )(rank, pw, root)


def panel_kernel(pw_ref, root_ref, out_ref, w2_ref):
    load_tables(pw_ref, w2_ref)
    parts, _, rows, _ = pw_ref.shape
    count = 16
    c = column(root_ref[0:1, :])[:count]
    t = column(root_ref[1:2, :])[:count]
    unroll = 16
    per_part = rows // unroll

    def sums_at(t):
        def body(r, sums):
            first, second, nearest = sums
            part = r // per_part
            start = (r % per_part) * unroll
            for u in range(unroll):
                distance = (pw_ref[part, 0, pl.ds(start + u, 1), :] - c) - t
                inverse = 1.0 / distance
                weighted = w2_ref[pl.ds(r * unroll + u, 1), :] * inverse
                first = first + weighted
                second = second + weighted * inverse
                nearest = jnp.minimum(nearest, jnp.abs(distance))
            return first, second, nearest

        zero = jnp.zeros((count, LANES), F32)
        first, second, nearest = lax.fori_loop(
            0, parts * per_part, body, (zero, zero, jnp.full((count, LANES), 3e38, F32))
        )
        return (
            jnp.sum(first, axis=1, keepdims=True),
            jnp.sum(second, axis=1, keepdims=True),
            jnp.min(nearest, axis=1, keepdims=True),
        )

    for _ in range(ITERS):
        sum_inverse, sum_square, nearest = sums_at(t)
        limit = 0.5 * nearest
        t = t - jnp.clip((1.0 + sum_inverse) / sum_square, -limit, limit)
    norm = lax.rsqrt(sums_at(t)[1])
    pad = jnp.zeros((LANES - count, LANES), F32)
    out_ref[0:1, :] = jnp.concatenate([t, pad], axis=0).T[0:1, :]
    out_ref[1:2, :] = jnp.concatenate([jnp.broadcast_to(norm, (count, LANES)), pad], axis=0).T[0:1, :]


def panel_roots(pw, root):
    n_pole_rows = pw.shape[0] * pw.shape[2]
    return pl.pallas_call(
        panel_kernel,
        out_shape=jax.ShapeDtypeStruct((2, LANES), F32),
        scratch_shapes=[pltpu.VMEM((n_pole_rows, LANES), F32)],
        cost_estimate=cost(4 * 20 * n_pole_rows * LANES * 10),
        name="panel_roots",
    )(pw, root)


def pick_kernel(index_ref, pw_ref, out_ref):
    parts, _, rows, _ = pw_ref.shape
    index = jnp.concatenate([index_ref[...], index_ref[...]], axis=0)
    row = index // LANES
    lane = index % LANES
    unroll = 16
    per_part = rows // unroll

    def body(r, carry):
        p, w = carry
        part = r // per_part
        start = (r % per_part) * unroll
        for u in range(unroll):
            hit = row == r * unroll + u
            p_row = jnp.broadcast_to(pw_ref[part, 0, pl.ds(start + u, 1), :], (8, LANES))
            w_row = jnp.broadcast_to(pw_ref[part, 1, pl.ds(start + u, 1), :], (8, LANES))
            p = jnp.where(hit, jnp.take_along_axis(p_row, lane, axis=1), p)
            w = jnp.where(hit, jnp.take_along_axis(w_row, lane, axis=1), w)
        return p, w

    zero = jnp.zeros((8, LANES), F32)
    p, w = lax.fori_loop(0, parts * per_part, body, (zero, zero))
    out_ref[0] = p[:4]
    out_ref[1] = w[:4]


def pick_columns(index, pw):
    return pl.pallas_call(
        pick_kernel,
        out_shape=jax.ShapeDtypeStruct((2, 4, LANES), F32),
        cost_estimate=cost(5e7),
        name="pick_columns",
    )(index, pw)


def matmul_kernel(col_ref, root_ref, *refs):
    blocks = refs[:8]
    own_ref, send_ref, p_ref, w_ref = refs[8:]
    sources = 4
    rows, depth = blocks[0].shape
    chunk = 256
    chunks = root_ref.shape[1] // chunk
    pieces = depth // LANES
    for src in range(sources):
        p = jnp.concatenate([col_ref[0, src]] * (LANES // pieces), axis=0).T
        w = jnp.concatenate([col_ref[1, src]] * (LANES // pieces), axis=0).T
        for piece in range(pieces):
            here = pl.ds(src * depth + piece * LANES, LANES)
            p_ref[here, :] = jnp.broadcast_to(p[:, piece : piece + 1], (LANES, LANES))
            w_ref[here, :] = jnp.broadcast_to(w[:, piece : piece + 1], (LANES, LANES))

    def cauchy(src, k):
        down = []
        for piece in range(pieces):
            here = pl.ds(src * depth + piece * LANES, LANES)
            p = p_ref[here, :]
            w = w_ref[here, :]
            across = []
            for part in range(chunk // LANES):
                lanes = pl.ds(k * chunk + part * LANES, LANES)
                distance = (p - root_ref[0:1, lanes]) - root_ref[1:2, lanes]
                value = w * (1.0 / distance) * root_ref[2:3, lanes]
                across.append(value.astype(BF16))
            down.append(jnp.concatenate(across, axis=1))
        return jnp.concatenate(down, axis=0)

    def body(k, carry):
        acc = None
        for src in range(sources):
            left = jnp.concatenate([blocks[src][...], blocks[sources + src][...]], axis=0)
            product = jnp.dot(left, cauchy(src, k), preferred_element_type=F32)
            acc = product if acc is None else acc + product
        quarter = rows // 4
        for part in range(4):
            for side in range(2):
                first = side * rows + part * quarter
                piece = acc[first : first + quarter]
                own_ref[part, side, :, pl.ds(k * chunk, chunk)] = piece
                send_ref[part, side, :, pl.ds(k * chunk, chunk)] = piece.astype(BF16)
        return carry

    lax.fori_loop(0, chunks, body, 0)


def panel_product(columns, root, blocks):
    sources = 4
    rows, depth = blocks[0].shape
    n_roots = root.shape[1]
    pieces = depth // LANES
    shape = (4, 2, rows // 4, n_roots)
    return pl.pallas_call(
        matmul_kernel,
        out_shape=(jax.ShapeDtypeStruct(shape, F32), jax.ShapeDtypeStruct(shape, BF16)),
        scratch_shapes=[pltpu.VMEM((sources * depth, LANES), F32)] * 2,
        compiler_params=pltpu.CompilerParams(vmem_limit_bytes=56 << 20),
        cost_estimate=cost(2 * 2 * sources * rows * depth * n_roots),
        name="panel_product",
    )(columns.reshape(2, sources, pieces, LANES), root, *blocks)


def copies(value, axis):
    size = lax.axis_size(axis)
    return lax.all_to_all(
        jnp.broadcast_to(value[None], (size, *value.shape)), axis, 0, 0, tiled=True
    )


def ring(shift):
    return [(i, (i + shift) % 4) for i in range(4)]


def merge(pole_values, weights, centers, offsets, chosen, column_pole, eigen_blocks):
    z = lax.axis_index("z")
    x = lax.axis_index("x")
    core = lax.axis_index("core")
    row = z * 4 + x
    col = lax.axis_index("y") * 2 + core
    n_col = centers.shape[0]
    n_own = n_col // 16
    swap = [(0, 1), (1, 0)]

    parted = jnp.stack([pole_values.reshape(-1, LANES), weights.reshape(-1, LANES)])
    pw = copies(parted, ROW)

    axes = ("z", "x")
    places = (z, x)
    wide = eigen_blocks.reshape(4, 4, -1, 2, eigen_blocks.shape[2])
    turned = (
        wide[:, :, :, 0].reshape(4, -1, eigen_blocks.shape[2]),
        jnp.swapaxes(wide[:, :, :, 1], 0, 1).reshape(4, -1, eigen_blocks.shape[2]),
    )
    cut = [
        [
            lax.dynamic_index_in_dim(turned[half], (places[half] + shift) % 4, 0, keepdims=False)
            for shift in range(4)
        ]
        for half in range(2)
    ]

    wanted = lax.dynamic_slice_in_dim(chosen, row * LANES, LANES)
    local = wanted - col * n_col
    hit = local[:, None] == lax.broadcasted_iota(jnp.int32, (1, n_col), 1)
    first = jnp.stack(
        [
            jnp.sum(jnp.where(hit, centers[None, :], 0.0), axis=1),
            jnp.sum(jnp.where(hit, offsets[None, :], 0.0), axis=1),
        ]
    )
    spread = jnp.moveaxis(first.reshape(2, 8, 16), 1, 0)
    pw, spread = lax.optimization_barrier((pw, spread))
    arrived = lax.all_to_all(spread, COL, 0, 0, tiled=True)
    index = lax.dynamic_slice_in_dim(column_pole.reshape(-1, LANES), col * 4, 4)
    picked = pick_columns(index, pw)
    cut, arrived = lax.optimization_barrier((cut, arrived))

    eigen = [[cut[0][0]], [cut[1][0]]]
    for shift in (1, 2, 3):
        for half in range(2):
            eigen[half].append(lax.ppermute(cut[half][shift], axes[half], ring(shift)))
    peer = [[lax.ppermute(eigen[half][0], "core", swap)] for half in range(2)]

    panel_start = jnp.pad(
        jnp.sum(arrived, axis=0), ((0, 0), (0, LANES - 16)), constant_values=0.25
    )
    panel_end = panel_roots(pw, panel_start)
    note = jnp.concatenate([picked.reshape(8, LANES), panel_start[:1], panel_end], axis=0)
    notes = copies(note, ALL)

    start = col * n_col + row * n_own
    my_centers = lax.dynamic_slice_in_dim(centers, row * n_own, n_own)
    my_offsets = lax.dynamic_slice_in_dim(offsets, row * n_own, n_own)
    part = start // pole_values.shape[0]
    own_poles = lax.dynamic_slice(
        pw.reshape(16, 2, -1), (part, 0, start - part * pole_values.shape[0]), (1, 1, n_own)
    ).reshape(n_own)
    low = own_poles - my_centers
    last = start + jnp.arange(n_own) == pole_values.shape[0] * 16 - 1
    high = jnp.where(last, 3e38, -low)
    state = jnp.stack([my_centers, my_offsets, low, high]).reshape(4, -1, GROUP)
    rank = start.reshape(1)
    roots_a = find_roots(rank, pw, state[:, :CUT_A])
    eigen, notes, roots_a = lax.optimization_barrier((eigen, notes, roots_a))

    for half in range(2):
        peer[half] += [lax.ppermute(block, "core", swap) for block in eigen[half][1:]]
    roots_b = find_roots(rank + CUT_A * GROUP, pw, state[:, CUT_A:CUT_B])

    table = notes[:, :8].reshape(4, 4, 2, 4, 2, 4, LANES)
    columns = (
        lax.dynamic_index_in_dim(table[:, :, 0], x, 1, keepdims=False),
        lax.dynamic_index_in_dim(table[:, :, 1], z, 0, keepdims=False),
    )
    columns = [
        jnp.moveaxis(
            jnp.concatenate(
                [lax.dynamic_slice_in_dim(c, (place - s) % 4, 1) for s in range(4)]
            ),
            2,
            0,
        ).reshape(2, -1, LANES)
        for c, place in zip(columns, places)
    ]
    panel_root = jnp.moveaxis(notes[:, 8:, :16], 1, 0).reshape(3, 2, -1)
    panel_root = lax.dynamic_index_in_dim(panel_root, core, 1, keepdims=False)
    panel_root, columns, peer, roots_b = lax.optimization_barrier(
        (panel_root, columns, peer, roots_b)
    )
    pieces = []
    for half in range(2):
        own, send = panel_product(columns[half], panel_root, eigen[half] + peer[half])
        other = places[1 - half]
        pieces.append([lax.dynamic_index_in_dim(own, other, 0, keepdims=False)])
        for shift in (1, 2, 3):
            piece = lax.dynamic_index_in_dim(send, (other + shift) % 4, 0, keepdims=False)
            pieces[half].append(lax.ppermute(piece, axes[1 - half], ring(shift)))
    roots_c = find_roots(rank + CUT_B * GROUP, pw, state[:, CUT_B:])
    total = jnp.stack([p[0] + p[1] + p[2] + p[3] for p in pieces])
    keep = total[:, 0]
    got = lax.ppermute(total[:, 1], "core", swap)
    roots = copies(jnp.concatenate([roots_a, roots_b, roots_c]), ROW)
    panel = jnp.where(
        core == 0, jnp.concatenate([keep, got], axis=2), jnp.concatenate([got, keep], axis=2)
    )
    return roots.reshape(-1), jnp.moveaxis(panel, 0, 1)


def solution(mesh):
    torus = Mesh(mesh.devices.reshape(4, 4, 4, 2), ALL)
    placed = (P(ROW), P(ROW), P(COL), P(COL), P(), P(None, ROW), P(COL, None, ROW))
    return jax.shard_map(
        merge,
        mesh=torus,
        in_specs=placed,
        out_specs=(P(COL), P(COL + ROW, None, None)),
        check_vma=False,
    )
```

```python
import jax
import jax.numpy as jnp
from jax import lax
from jax.experimental import pallas as pl
from jax.experimental.pallas import tpu as pltpu
from jax.sharding import Mesh
from jax.sharding import PartitionSpec as P

ITERS = 3
ROW = ("z", "x")
COL = ("y", "core")
ALL = ("z", "x", "y", "core")
F32 = jnp.float32
BF16 = jnp.bfloat16
LANES = 128
GROUP = 128
BLOCK = 16
CUT_A = 2
CUT_B = 3


def cost(flops):
    return pl.CostEstimate(flops=int(flops), bytes_accessed=1 << 20, transcendentals=0)


def column(row):
    return jnp.broadcast_to(row, (LANES, LANES)).T


def root_kernel(rank_ref, pw_ref, root_ref, out_ref, w2_ref, ps_ref, c_ref, t_ref, lo_ref, hi_ref):
    w2_ref[...] = pw_ref[1] * pw_ref[1]
    groups = root_ref.shape[1]
    blocks = ps_ref.shape[0] // BLOCK
    for k in range(groups):
        here = pl.ds(k * GROUP, GROUP)
        c_ref[here, :] = column(root_ref[0, k : k + 1, :])
        t_ref[here, :] = column(root_ref[1, k : k + 1, :])
        lo_ref[here, :] = column(root_ref[2, k : k + 1, :])
        hi_ref[here, :] = column(root_ref[3, k : k + 1, :])

    def group_body(g, carry):
        here = pl.ds(g * GROUP, GROUP)
        base = c_ref[pl.ds(g * GROUP + GROUP // 2, 1), :]
        ps_ref[...] = pw_ref[0] - base
        offset = c_ref[here, :] - base
        near_block = jnp.clip((rank_ref[0] // LANES + g - BLOCK // 2) // BLOCK, 0, blocks - 2)

        def step(_, carry):
            t = t_ref[here, :]
            s = offset + t

            def near(r, sums):
                first, second = sums
                for u in range(BLOCK):
                    row = pl.ds((near_block + r) * BLOCK + u, 1)
                    inverse = 1.0 / (ps_ref[row, :] - s)
                    weighted = w2_ref[row, :] * inverse
                    first = first + weighted
                    second = second + weighted * inverse
                return first, second

            def far(i, sums):
                first, second = sums
                for half in range(2):
                    block = 2 * i + half
                    block = jnp.where(block >= near_block, block + 2, block)
                    some = None
                    for u in range(BLOCK):
                        row = pl.ds(block * BLOCK + u, 1)
                        distance = (ps_ref[row, :] - s).astype(BF16)
                        weight = jnp.broadcast_to(w2_ref[row, :], (GROUP, LANES)).astype(BF16)
                        weighted = weight / distance
                        square = weighted / distance
                        some = (weighted, square) if some is None else (some[0] + weighted, some[1] + square)
                    first = first + some[0].astype(F32)
                    second = second + some[1].astype(F32)
                return first, second

            zero = jnp.zeros((GROUP, LANES), F32)
            sums = lax.fori_loop(0, 2, near, (zero, zero))
            first, second = lax.fori_loop(0, (blocks - 2) // 2, far, sums)
            sum_inverse = jnp.sum(first, axis=1, keepdims=True)
            sum_square = jnp.sum(second, axis=1, keepdims=True)
            nearest = jnp.minimum(jnp.abs(lo_ref[here, :] - t), jnp.abs(hi_ref[here, :] - t))
            limit = 0.5 * nearest
            t_ref[here, :] = t - jnp.clip((1.0 + sum_inverse) / sum_square, -limit, limit)
            return carry

        lax.fori_loop(0, ITERS, step, 0)
        return carry

    lax.fori_loop(0, groups, group_body, 0)
    for k in range(groups):
        out_ref[k : k + 1, :] = t_ref[pl.ds(k * GROUP, GROUP), :].T[0:1, :]


def find_roots(rank, pw, root):
    groups = root.shape[1]
    n_pole_rows = pw.shape[1]
    roots = groups * GROUP
    vmem = pl.BlockSpec(memory_space=pltpu.VMEM)
    return pl.pallas_call(
        root_kernel,
        in_specs=[pl.BlockSpec(memory_space=pltpu.SMEM), vmem, vmem],
        out_shape=jax.ShapeDtypeStruct((groups, LANES), F32),
        scratch_shapes=[pltpu.VMEM((n_pole_rows, LANES), F32)] * 2
        + [pltpu.VMEM((roots, LANES), F32)] * 4,
        cost_estimate=cost(ITERS * roots * n_pole_rows * LANES * 10),
        name="find_roots",
    )(rank, pw, root)


def panel_kernel(pw_ref, root_ref, out_ref, w2_ref):
    w2_ref[...] = pw_ref[1] * pw_ref[1]
    count = 16
    c = column(root_ref[0:1, :])[:count]
    t = column(root_ref[1:2, :])[:count]
    unroll = 32
    zero = jnp.zeros((count, LANES), F32)

    def sums_at(t):
        def body(r, sums):
            first, second, nearest = sums
            for u in range(unroll):
                row = pl.ds(r * unroll + u, 1)
                distance = (pw_ref[0, row, :] - c) - t
                inverse = 1.0 / distance
                weighted = w2_ref[row, :] * inverse
                first = first + weighted
                second = second + weighted * inverse
                nearest = jnp.minimum(nearest, jnp.abs(distance))
            return first, second, nearest

        first, second, nearest = lax.fori_loop(
            0, w2_ref.shape[0] // unroll, body, (zero, zero, jnp.full((count, LANES), 3e38, F32))
        )
        return (
            jnp.sum(first, axis=1, keepdims=True),
            jnp.sum(second, axis=1, keepdims=True),
            jnp.min(nearest, axis=1, keepdims=True),
        )

    for _ in range(ITERS):
        sum_inverse, sum_square, nearest = sums_at(t)
        limit = 0.5 * nearest
        t = t - jnp.clip((1.0 + sum_inverse) / sum_square, -limit, limit)
    norm = lax.rsqrt(sums_at(t)[1])
    pad = jnp.zeros((LANES - count, LANES), F32)
    out_ref[0:1, :] = jnp.concatenate([t, pad], axis=0).T[0:1, :]
    out_ref[1:2, :] = jnp.concatenate([jnp.broadcast_to(norm, (count, LANES)), pad], axis=0).T[0:1, :]


def panel_roots(pw, root):
    n_pole_rows = pw.shape[1]
    return pl.pallas_call(
        panel_kernel,
        out_shape=jax.ShapeDtypeStruct((2, LANES), F32),
        scratch_shapes=[pltpu.VMEM((n_pole_rows, LANES), F32)],
        cost_estimate=cost(4 * 20 * n_pole_rows * LANES * 10),
        name="panel_roots",
    )(pw, root)


def pick_kernel(index_ref, pw_ref, out_ref):
    index = jnp.concatenate([index_ref[...], index_ref[...]], axis=0)
    row = index // LANES
    lane = index % LANES
    unroll = 16

    def body(r, carry):
        p, w = carry
        for u in range(unroll):
            at = r * unroll + u
            hit = row == at
            p_row = jnp.broadcast_to(pw_ref[0, pl.ds(at, 1), :], (8, LANES))
            w_row = jnp.broadcast_to(pw_ref[1, pl.ds(at, 1), :], (8, LANES))
            p = jnp.where(hit, jnp.take_along_axis(p_row, lane, axis=1), p)
            w = jnp.where(hit, jnp.take_along_axis(w_row, lane, axis=1), w)
        return p, w

    zero = jnp.zeros((8, LANES), F32)
    p, w = lax.fori_loop(0, pw_ref.shape[1] // unroll, body, (zero, zero))
    out_ref[0] = p[:4]
    out_ref[1] = w[:4]


def pick_columns(index, pw):
    return pl.pallas_call(
        pick_kernel,
        out_shape=jax.ShapeDtypeStruct((2, 4, LANES), F32),
        cost_estimate=cost(5e7),
        name="pick_columns",
    )(index, pw)


def matmul_kernel(place_ref, col_ref, root_ref, *refs):
    blocks = refs[:16]
    outs = refs[16:24]
    p_ref, w_ref, e_ref, acc_ref, sems = refs[24:]
    sources = 4
    halves, _, both, depth = e_ref.shape
    rows = both // 2
    quarter = rows // 4
    n_roots = root_ref.shape[1]
    pieces = depth // LANES

    def moves(half, src):
        return [
            pltpu.make_async_copy(
                blocks[half * 8 + side * 4 + src],
                e_ref.at[half, src, pl.ds(side * rows, rows)],
                sems.at[half, src, side],
            )
            for side in range(2)
        ]

    for half in range(halves):
        for src in range(sources):
            for move in moves(half, src):
                move.start()

    def half_body(half, carry):
        for src in range(sources):
            p = jnp.concatenate([col_ref[half, 0, src]] * (LANES // pieces), axis=0).T
            w = jnp.concatenate([col_ref[half, 1, src]] * (LANES // pieces), axis=0).T
            for piece in range(pieces):
                here = pl.ds(src * depth + piece * LANES, LANES)
                p_ref[here, :] = jnp.broadcast_to(p[:, piece : piece + 1], (LANES, LANES))
                w_ref[here, :] = jnp.broadcast_to(w[:, piece : piece + 1], (LANES, LANES))
        for which in range(halves):

            @pl.when(half == which)
            def _():
                for src in range(sources):
                    for move in moves(which, src):
                        move.wait()

        def cauchy(src):
            down = []
            for piece in range(pieces):
                here = pl.ds(src * depth + piece * LANES, LANES)
                p = p_ref[here, :]
                w = w_ref[here, :]
                across = []
                for part in range(n_roots // LANES):
                    lanes = pl.ds(part * LANES, LANES)
                    distance = (p - root_ref[0:1, lanes]) - root_ref[1:2, lanes]
                    value = w * (1.0 / distance) * root_ref[2:3, lanes]
                    across.append(value.astype(BF16))
                down.append(jnp.concatenate(across, axis=1))
            return jnp.concatenate(down, axis=0)

        acc = None
        for src in range(sources):
            product = jnp.dot(e_ref[half, src], cauchy(src), preferred_element_type=F32)
            acc = product if acc is None else acc + product
        acc_ref[...] = acc
        for which in range(halves):

            @pl.when(half == which)
            def _():
                for shift in range(4):
                    part = (place_ref[which] + shift) % 4
                    for side in range(2):
                        piece = acc_ref[pl.ds(side * rows + part * quarter, quarter), :]
                        out = outs[which * 4 + shift]
                        out[side] = piece.astype(out.dtype)

        return carry

    lax.fori_loop(0, halves, half_body, 0)


def panel_product(places, columns, root, blocks):
    rows, depth = blocks[0].shape
    n_roots = root.shape[1]
    shape = (2, rows // 4, n_roots)
    types = [F32, BF16, BF16, BF16] * 2
    vmem = pl.BlockSpec(memory_space=pltpu.VMEM)
    return pl.pallas_call(
        matmul_kernel,
        in_specs=[pl.BlockSpec(memory_space=pltpu.SMEM), vmem, vmem] + [pl.BlockSpec(memory_space=pl.ANY)] * 16,
        out_shape=[jax.ShapeDtypeStruct(shape, t) for t in types],
        scratch_shapes=[pltpu.VMEM((4 * depth, LANES), F32)] * 2
        + [
            pltpu.VMEM((2, 4, 2 * rows, depth), BF16),
            pltpu.VMEM((2 * rows, n_roots), F32),
            pltpu.SemaphoreType.DMA((2, 4, 2)),
        ],
        cost_estimate=cost(2 * 16 * rows * depth * n_roots),
        compiler_params=pltpu.CompilerParams(vmem_limit_bytes=56 << 20),
        name="panel_product",
    )(places, columns, root, *blocks)


def copies(value, axis):
    size = lax.axis_size(axis)
    return lax.all_to_all(
        jnp.broadcast_to(value[None], (size, *value.shape)), axis, 0, 0, tiled=True
    )


def ring(shift):
    return [(i, (i + shift) % 4) for i in range(4)]


def merge(pole_values, weights, centers, offsets, chosen, column_pole, eigen_blocks):
    z = lax.axis_index("z")
    x = lax.axis_index("x")
    core = lax.axis_index("core")
    row = z * 4 + x
    col = lax.axis_index("y") * 2 + core
    n_col = centers.shape[0]
    n_own = n_col // 16
    swap = [(0, 1), (1, 0)]

    wanted = lax.dynamic_slice_in_dim(chosen, row * LANES, LANES)
    local = wanted - col * n_col
    hit = local[:, None] == lax.broadcasted_iota(jnp.int32, (1, n_col), 1)
    first = jnp.stack(
        [
            jnp.sum(jnp.where(hit, centers[None, :], 0.0), axis=1),
            jnp.sum(jnp.where(hit, offsets[None, :], 0.0), axis=1),
        ]
    )
    spread = jnp.moveaxis(first.reshape(2, 8, 16), 1, 0).reshape(8, 1, 32)
    spread = jnp.tile(jnp.pad(spread, ((0, 0), (0, 0), (0, LANES - 32))), (16, 1, 1))
    part = jnp.concatenate(
        [
            lax.dynamic_slice_in_dim(v.reshape(-1, LANES), col * 4, 4)
            for v in (pole_values, weights)
        ]
    )
    out = jnp.concatenate([jnp.broadcast_to(part[None], (128, 8, LANES)), spread], axis=1)
    arrived = lax.all_to_all(out, ALL, 0, 0, tiled=True)

    axes = ("z", "x")
    places = (z, x)
    wide = eigen_blocks.reshape(4, 4, -1, 2, eigen_blocks.shape[2])
    turned = (
        wide[:, :, :, 0].reshape(4, -1, eigen_blocks.shape[2]),
        jnp.swapaxes(wide[:, :, :, 1], 0, 1).reshape(4, -1, eigen_blocks.shape[2]),
    )
    cut = [
        [
            lax.dynamic_index_in_dim(turned[half], (places[half] + shift) % 4, 0, keepdims=False)
            for shift in range(4)
        ]
        for half in range(2)
    ]

    cut, arrived = lax.optimization_barrier((cut, arrived))
    eigen = [[cut[0][0]], [cut[1][0]]]
    for shift in (1, 2, 3):
        for half in range(2):
            eigen[half].append(lax.ppermute(cut[half][shift], axes[half], ring(shift)))
    peer = [[lax.ppermute(eigen[half][0], "core", swap)] for half in range(2)]

    pw = jnp.moveaxis(arrived[:, :8].reshape(128, 2, 4, LANES), 1, 0).reshape(2, -1, LANES)
    begun = lax.dynamic_slice(arrived, (row * 8, 8, 0), (8, 1, 32))
    panel_start = jnp.pad(
        jnp.sum(begun, axis=(0, 1)).reshape(2, 16),
        ((0, 0), (0, LANES - 16)),
        constant_values=0.25,
    )
    panel_end = panel_roots(pw, panel_start)
    index = lax.dynamic_slice_in_dim(column_pole.reshape(-1, LANES), col * 4, 4)
    picked = pick_columns(index, pw)
    note = jnp.concatenate([picked.reshape(8, LANES), panel_start[:1], panel_end], axis=0)
    notes = copies(note, ALL)

    start = col * n_col + row * n_own
    my_centers = lax.dynamic_slice_in_dim(centers.reshape(-1, LANES), row * 4, 4)
    my_offsets = lax.dynamic_slice_in_dim(offsets.reshape(-1, LANES), row * 4, 4)
    own_poles = lax.dynamic_slice_in_dim(pw[0], start // LANES, 4)
    low = own_poles - my_centers
    ranks = start + jnp.arange(n_own).reshape(-1, LANES)
    high = jnp.where(ranks == pw[0].size - 1, 3e38, -low)
    state = jnp.stack([my_centers, my_offsets, low, high])
    rank = start.reshape(1)
    roots_a = find_roots(rank, pw, state[:, :CUT_A])
    eigen, notes, roots_a = lax.optimization_barrier((eigen, notes, roots_a))

    for half in range(2):
        peer[half] += [lax.ppermute(block, "core", swap) for block in eigen[half][1:]]
    roots_b = find_roots(rank + CUT_A * GROUP, pw, state[:, CUT_A:CUT_B])

    table = notes[:, :8].reshape(4, 4, 2, 4, 2, 4, LANES)
    columns = (
        lax.dynamic_index_in_dim(table[:, :, 0], x, 1, keepdims=False),
        lax.dynamic_index_in_dim(table[:, :, 1], z, 0, keepdims=False),
    )
    columns = [
        jnp.moveaxis(
            jnp.concatenate(
                [lax.dynamic_slice_in_dim(c, (place - s) % 4, 1) for s in range(4)]
            ),
            2,
            0,
        ).reshape(2, 4, -1, LANES)
        for c, place in zip(columns, places)
    ]
    panel_root = jnp.moveaxis(notes[:, 8:, :16], 1, 0).reshape(3, 2, -1)
    panel_root = lax.dynamic_index_in_dim(panel_root, core, 1, keepdims=False)
    panel_root, columns, peer, roots_b = lax.optimization_barrier(
        (panel_root, columns, peer, roots_b)
    )
    sums = panel_product(
        jnp.stack([x, z]).astype(jnp.int32),
        jnp.stack(columns),
        panel_root,
        eigen[0] + peer[0] + eigen[1] + peer[1],
    )
    pieces = []
    for half in range(2):
        mine = sums[4 * half : 4 * half + 4]
        pieces.append(
            [mine[0]]
            + [lax.ppermute(mine[s], axes[1 - half], ring(s)) for s in (1, 2, 3)]
        )
    roots_c = find_roots(rank + CUT_B * GROUP, pw, state[:, CUT_B:])

    def added(side):
        return jnp.stack([p[0][side] + p[1][side] + p[2][side] + p[3][side] for p in pieces])

    roots = copies(jnp.concatenate([roots_a, roots_b, roots_c]), ROW)
    got = lax.ppermute(added(1), "core", swap)
    keep = added(0)
    panel = jnp.where(
        core == 0, jnp.concatenate([keep, got], axis=2), jnp.concatenate([got, keep], axis=2)
    )
    return roots.reshape(-1), jnp.moveaxis(panel, 0, 1)


def solution(mesh):
    torus = Mesh(mesh.devices.reshape(4, 4, 4, 2), ALL)
    placed = (P(ROW), P(ROW), P(COL), P(COL), P(), P(None, ROW), P(COL, None, ROW))
    return jax.shard_map(
        merge,
        mesh=torus,
        in_specs=placed,
        out_specs=(P(COL), P(COL + ROW, None, None)),
        check_vma=False,
    )
```

```python
import jax
import jax.numpy as jnp
from jax import lax
from jax.experimental import pallas as pl
from jax.experimental.pallas import tpu as pltpu
from jax.sharding import Mesh
from jax.sharding import PartitionSpec as P

ITERS = 3
ROW = ("z", "x")
COL = ("y", "core")
ALL = ("z", "x", "y", "core")
F32 = jnp.float32
BF16 = jnp.bfloat16
LANES = 128
GROUP = 128
BLOCK = 16
CUT_A = 2
CUT_B = 3


def cost(flops):
    return pl.CostEstimate(flops=int(flops), bytes_accessed=1 << 20, transcendentals=0)


def column(row):
    return jnp.broadcast_to(row, (LANES, LANES)).T


def root_kernel(rank_ref, pw_ref, root_ref, out_ref, w2_ref, ps_ref, c_ref, t_ref, lo_ref, hi_ref):
    w2_ref[...] = pw_ref[1] * pw_ref[1]
    groups = root_ref.shape[1]
    blocks = ps_ref.shape[0] // BLOCK
    for k in range(groups):
        here = pl.ds(k * GROUP, GROUP)
        c_ref[here, :] = column(root_ref[0, k : k + 1, :])
        t_ref[here, :] = column(root_ref[1, k : k + 1, :])
        lo_ref[here, :] = column(root_ref[2, k : k + 1, :])
        hi_ref[here, :] = column(root_ref[3, k : k + 1, :])

    def group_body(g, carry):
        here = pl.ds(g * GROUP, GROUP)
        base = c_ref[pl.ds(g * GROUP + GROUP // 2, 1), :]
        ps_ref[...] = pw_ref[0] - base
        offset = c_ref[here, :] - base
        near_block = jnp.clip((rank_ref[0] // LANES + g - BLOCK // 2) // BLOCK, 0, blocks - 2)

        def step(_, carry):
            t = t_ref[here, :]
            s = offset + t

            def near(r, sums):
                first, second = sums
                for u in range(BLOCK):
                    row = pl.ds((near_block + r) * BLOCK + u, 1)
                    inverse = 1.0 / (ps_ref[row, :] - s)
                    weighted = w2_ref[row, :] * inverse
                    first = first + weighted
                    second = second + weighted * inverse
                return first, second

            def far(i, sums):
                first, second = sums
                for half in range(2):
                    block = 2 * i + half
                    block = jnp.where(block >= near_block, block + 2, block)
                    some = None
                    for u in range(BLOCK):
                        row = pl.ds(block * BLOCK + u, 1)
                        distance = (ps_ref[row, :] - s).astype(BF16)
                        weight = jnp.broadcast_to(w2_ref[row, :], (GROUP, LANES)).astype(BF16)
                        weighted = weight / distance
                        square = weighted / distance
                        some = (weighted, square) if some is None else (some[0] + weighted, some[1] + square)
                    first = first + some[0].astype(F32)
                    second = second + some[1].astype(F32)
                return first, second

            zero = jnp.zeros((GROUP, LANES), F32)
            sums = lax.fori_loop(0, 2, near, (zero, zero))
            first, second = lax.fori_loop(0, (blocks - 2) // 2, far, sums)
            sum_inverse = jnp.sum(first, axis=1, keepdims=True)
            sum_square = jnp.sum(second, axis=1, keepdims=True)
            nearest = jnp.minimum(jnp.abs(lo_ref[here, :] - t), jnp.abs(hi_ref[here, :] - t))
            limit = 0.5 * nearest
            t_ref[here, :] = t - jnp.clip((1.0 + sum_inverse) / sum_square, -limit, limit)
            return carry

        lax.fori_loop(0, ITERS, step, 0)
        return carry

    lax.fori_loop(0, groups, group_body, 0)
    for k in range(groups):
        out_ref[k : k + 1, :] = t_ref[pl.ds(k * GROUP, GROUP), :].T[0:1, :]


def find_roots(rank, pw, root):
    groups = root.shape[1]
    n_pole_rows = pw.shape[1]
    roots = groups * GROUP
    vmem = pl.BlockSpec(memory_space=pltpu.VMEM)
    return pl.pallas_call(
        root_kernel,
        in_specs=[pl.BlockSpec(memory_space=pltpu.SMEM), vmem, vmem],
        out_shape=jax.ShapeDtypeStruct((groups, LANES), F32),
        scratch_shapes=[pltpu.VMEM((n_pole_rows, LANES), F32)] * 2
        + [pltpu.VMEM((roots, LANES), F32)] * 4,
        cost_estimate=cost(ITERS * roots * n_pole_rows * LANES * 10),
        name="find_roots",
    )(rank, pw, root)


def panel_kernel(pw_ref, root_ref, out_ref, w2_ref):
    w2_ref[...] = pw_ref[1] * pw_ref[1]
    count = 16
    c = column(root_ref[0:1, :])[:count]
    t = column(root_ref[1:2, :])[:count]
    unroll = 32
    zero = jnp.zeros((count, LANES), F32)

    def sums_at(t):
        def body(r, sums):
            first, second, nearest = sums
            for u in range(unroll):
                row = pl.ds(r * unroll + u, 1)
                distance = (pw_ref[0, row, :] - c) - t
                inverse = 1.0 / distance
                weighted = w2_ref[row, :] * inverse
                first = first + weighted
                second = second + weighted * inverse
                nearest = jnp.minimum(nearest, jnp.abs(distance))
            return first, second, nearest

        first, second, nearest = lax.fori_loop(
            0, w2_ref.shape[0] // unroll, body, (zero, zero, jnp.full((count, LANES), 3e38, F32))
        )
        return (
            jnp.sum(first, axis=1, keepdims=True),
            jnp.sum(second, axis=1, keepdims=True),
            jnp.min(nearest, axis=1, keepdims=True),
        )

    for _ in range(ITERS):
        sum_inverse, sum_square, nearest = sums_at(t)
        limit = 0.5 * nearest
        t = t - jnp.clip((1.0 + sum_inverse) / sum_square, -limit, limit)
    norm = lax.rsqrt(sums_at(t)[1])
    pad = jnp.zeros((LANES - count, LANES), F32)
    out_ref[0:1, :] = jnp.concatenate([t, pad], axis=0).T[0:1, :]
    out_ref[1:2, :] = jnp.concatenate([jnp.broadcast_to(norm, (count, LANES)), pad], axis=0).T[0:1, :]


def panel_roots(pw, root):
    n_pole_rows = pw.shape[1]
    return pl.pallas_call(
        panel_kernel,
        out_shape=jax.ShapeDtypeStruct((2, LANES), F32),
        scratch_shapes=[pltpu.VMEM((n_pole_rows, LANES), F32)],
        cost_estimate=cost(4 * 20 * n_pole_rows * LANES * 10),
        name="panel_roots",
    )(pw, root)


def pick_kernel(index_ref, pw_ref, out_ref):
    index = jnp.concatenate([index_ref[...], index_ref[...]], axis=0)
    row = index // LANES
    lane = index % LANES
    unroll = 16

    def body(r, carry):
        p, w = carry
        for u in range(unroll):
            at = r * unroll + u
            hit = row == at
            p_row = jnp.broadcast_to(pw_ref[0, pl.ds(at, 1), :], (8, LANES))
            w_row = jnp.broadcast_to(pw_ref[1, pl.ds(at, 1), :], (8, LANES))
            p = jnp.where(hit, jnp.take_along_axis(p_row, lane, axis=1), p)
            w = jnp.where(hit, jnp.take_along_axis(w_row, lane, axis=1), w)
        return p, w

    zero = jnp.zeros((8, LANES), F32)
    p, w = lax.fori_loop(0, pw_ref.shape[1] // unroll, body, (zero, zero))
    out_ref[0] = p[:4]
    out_ref[1] = w[:4]


def pick_columns(index, pw):
    return pl.pallas_call(
        pick_kernel,
        out_shape=jax.ShapeDtypeStruct((2, 4, LANES), F32),
        cost_estimate=cost(5e7),
        name="pick_columns",
    )(index, pw)


def turn_kernel(place_ref, in_ref, *refs):
    outs = refs[:8]
    wide_ref, half_ref, in_sems, out_sems = refs[8:]
    blocks, rows = wide_ref.shape[:2]

    def fetch(i):
        return pltpu.make_async_copy(in_ref.at[pl.ds(i * rows, rows)], wide_ref.at[i], in_sems.at[i])

    def leave(i, half, shift):
        first = (i % 4 if half == 0 else i // 4) * rows
        return pltpu.make_async_copy(
            half_ref.at[half, i], outs[half * 4 + shift].at[pl.ds(first, rows)], out_sems.at[half, i]
        )

    for i in range(blocks):
        fetch(i).start()

    def body(i, carry):
        fetch(i).wait()
        both = jnp.swapaxes(wide_ref[i], 0, 1)
        for half in range(2):
            half_ref[half, i] = both[half]
            to = ((i // 4 if half == 0 else i % 4) - place_ref[half] + 4) % 4
            for shift in range(4):

                @pl.when(to == shift)
                def _():
                    leave(i, half, shift).start()

        return carry

    lax.fori_loop(0, blocks, body, 0)

    def finish(i, carry):
        for half in range(2):
            leave(i, half, 0).wait()
        return carry

    lax.fori_loop(0, blocks, finish, 0)


def turn_blocks(places, wide):
    n, halves, depth = wide.shape
    rows = n // 16
    hbm = pl.BlockSpec(memory_space=pl.ANY)
    return pl.pallas_call(
        turn_kernel,
        in_specs=[pl.BlockSpec(memory_space=pltpu.SMEM), hbm],
        out_specs=[hbm] * 8,
        out_shape=[jax.ShapeDtypeStruct((n // 4, depth), BF16)] * 8,
        scratch_shapes=[
            pltpu.VMEM((16, rows, halves, depth), BF16),
            pltpu.VMEM((halves, 16, rows, depth), BF16),
            pltpu.SemaphoreType.DMA((16,)),
            pltpu.SemaphoreType.DMA((halves, 16)),
        ],
        cost_estimate=cost(5e7),
        name="turn_blocks",
    )(places, wide)


def matmul_kernel(place_ref, col_ref, root_ref, *refs):
    blocks = refs[:16]
    outs = refs[16:24]
    p_ref, w_ref, e_ref, acc_ref, sems = refs[24:]
    sources = 4
    halves, _, both, depth = e_ref.shape
    rows = both // 2
    quarter = rows // 4
    n_roots = root_ref.shape[1]
    pieces = depth // LANES

    def moves(half, src):
        return [
            pltpu.make_async_copy(
                blocks[half * 8 + side * 4 + src],
                e_ref.at[half, src, pl.ds(side * rows, rows)],
                sems.at[half, src, side],
            )
            for side in range(2)
        ]

    for half in range(halves):
        for src in range(sources):
            for move in moves(half, src):
                move.start()

    def half_body(half, carry):
        for src in range(sources):
            p = jnp.concatenate([col_ref[half, 0, src]] * (LANES // pieces), axis=0).T
            w = jnp.concatenate([col_ref[half, 1, src]] * (LANES // pieces), axis=0).T
            for piece in range(pieces):
                here = pl.ds(src * depth + piece * LANES, LANES)
                p_ref[here, :] = jnp.broadcast_to(p[:, piece : piece + 1], (LANES, LANES))
                w_ref[here, :] = jnp.broadcast_to(w[:, piece : piece + 1], (LANES, LANES))
        for which in range(halves):

            @pl.when(half == which)
            def _():
                for src in range(sources):
                    for move in moves(which, src):
                        move.wait()

        def cauchy(src):
            down = []
            for piece in range(pieces):
                here = pl.ds(src * depth + piece * LANES, LANES)
                p = p_ref[here, :]
                w = w_ref[here, :]
                across = []
                for part in range(n_roots // LANES):
                    lanes = pl.ds(part * LANES, LANES)
                    distance = (p - root_ref[0:1, lanes]) - root_ref[1:2, lanes]
                    value = w * (1.0 / distance) * root_ref[2:3, lanes]
                    across.append(value.astype(BF16))
                down.append(jnp.concatenate(across, axis=1))
            return jnp.concatenate(down, axis=0)

        acc = None
        for src in range(sources):
            product = jnp.dot(e_ref[half, src], cauchy(src), preferred_element_type=F32)
            acc = product if acc is None else acc + product
        acc_ref[...] = acc
        for which in range(halves):

            @pl.when(half == which)
            def _():
                for shift in range(4):
                    part = (place_ref[which] + shift) % 4
                    for side in range(2):
                        piece = acc_ref[pl.ds(side * rows + part * quarter, quarter), :]
                        out = outs[which * 4 + shift]
                        out[side] = piece.astype(out.dtype)

        return carry

    lax.fori_loop(0, halves, half_body, 0)


def panel_product(places, columns, root, blocks):
    rows, depth = blocks[0].shape
    n_roots = root.shape[1]
    shape = (2, rows // 4, n_roots)
    types = [F32, BF16, BF16, BF16] * 2
    vmem = pl.BlockSpec(memory_space=pltpu.VMEM)
    return pl.pallas_call(
        matmul_kernel,
        in_specs=[pl.BlockSpec(memory_space=pltpu.SMEM), vmem, vmem] + [pl.BlockSpec(memory_space=pl.ANY)] * 16,
        out_shape=[jax.ShapeDtypeStruct(shape, t) for t in types],
        scratch_shapes=[pltpu.VMEM((4 * depth, LANES), F32)] * 2
        + [
            pltpu.VMEM((2, 4, 2 * rows, depth), BF16),
            pltpu.VMEM((2 * rows, n_roots), F32),
            pltpu.SemaphoreType.DMA((2, 4, 2)),
        ],
        cost_estimate=cost(2 * 16 * rows * depth * n_roots),
        compiler_params=pltpu.CompilerParams(vmem_limit_bytes=56 << 20),
        name="panel_product",
    )(places, columns, root, *blocks)


def copies(value, axis):
    size = lax.axis_size(axis)
    return lax.all_to_all(
        jnp.broadcast_to(value[None], (size, *value.shape)), axis, 0, 0, tiled=True
    )


def ring(shift):
    return [(i, (i + shift) % 4) for i in range(4)]


def merge(pole_values, weights, centers, offsets, chosen, column_pole, eigen_blocks):
    z = lax.axis_index("z")
    x = lax.axis_index("x")
    core = lax.axis_index("core")
    row = z * 4 + x
    col = lax.axis_index("y") * 2 + core
    n_col = centers.shape[0]
    n_own = n_col // 16
    swap = [(0, 1), (1, 0)]

    parted = jnp.stack([pole_values.reshape(-1, LANES), weights.reshape(-1, LANES)])
    arrived = copies(parted, ROW)

    axes = ("z", "x")
    places = (z, x)
    cut = turn_blocks(jnp.stack(places).astype(jnp.int32), eigen_blocks)

    wanted = lax.dynamic_slice_in_dim(chosen, row * LANES, LANES)
    local = wanted - col * n_col
    hit = local[:, None] == lax.broadcasted_iota(jnp.int32, (1, n_col), 1)
    first = jnp.stack(
        [
            jnp.sum(jnp.where(hit, centers[None, :], 0.0), axis=1),
            jnp.sum(jnp.where(hit, offsets[None, :], 0.0), axis=1),
        ]
    )
    spread = jnp.moveaxis(first.reshape(2, 8, 16), 1, 0)
    arrived, cut, spread = lax.optimization_barrier((arrived, cut, spread))
    cut = (cut[:4], cut[4:])
    pw = jnp.moveaxis(arrived, 1, 0).reshape(2, -1, LANES)
    begun = lax.all_to_all(spread, COL, 0, 0, tiled=True)
    eigen = [[cut[0][0]], [cut[1][0]]]
    for shift in (1, 2, 3):
        for half in range(2):
            eigen[half].append(lax.ppermute(cut[half][shift], axes[half], ring(shift)))
    peer = [[lax.ppermute(eigen[half][0], "core", swap)] for half in range(2)]

    panel_start = jnp.pad(
        jnp.sum(begun, axis=0), ((0, 0), (0, LANES - 16)), constant_values=0.25
    )
    panel_end = panel_roots(pw, panel_start)
    index = lax.dynamic_slice_in_dim(column_pole.reshape(-1, LANES), col * 4, 4)
    picked = pick_columns(index, pw)
    note = jnp.concatenate([picked.reshape(8, LANES), panel_start[:1], panel_end], axis=0)
    notes = copies(note, ALL)

    start = col * n_col + row * n_own
    my_centers = lax.dynamic_slice_in_dim(centers.reshape(-1, LANES), row * 4, 4)
    my_offsets = lax.dynamic_slice_in_dim(offsets.reshape(-1, LANES), row * 4, 4)
    own_poles = lax.dynamic_slice_in_dim(pw[0], start // LANES, 4)
    low = own_poles - my_centers
    ranks = start + jnp.arange(n_own).reshape(-1, LANES)
    high = jnp.where(ranks == pw[0].size - 1, 3e38, -low)
    state = jnp.stack([my_centers, my_offsets, low, high])
    rank = start.reshape(1)
    roots_a = find_roots(rank, pw, state[:, :CUT_A])
    eigen, notes, roots_a = lax.optimization_barrier((eigen, notes, roots_a))

    for half in range(2):
        peer[half] += [lax.ppermute(block, "core", swap) for block in eigen[half][1:]]
    roots_b = find_roots(rank + CUT_A * GROUP, pw, state[:, CUT_A:CUT_B])

    table = notes[:, :8].reshape(4, 4, 2, 4, 2, 4, LANES)
    columns = (
        lax.dynamic_index_in_dim(table[:, :, 0], x, 1, keepdims=False),
        lax.dynamic_index_in_dim(table[:, :, 1], z, 0, keepdims=False),
    )
    columns = [
        jnp.moveaxis(
            jnp.concatenate(
                [lax.dynamic_slice_in_dim(c, (place - s) % 4, 1) for s in range(4)]
            ),
            2,
            0,
        ).reshape(2, 4, -1, LANES)
        for c, place in zip(columns, places)
    ]
    panel_root = jnp.moveaxis(notes[:, 8:, :16], 1, 0).reshape(3, 2, -1)
    panel_root = lax.dynamic_index_in_dim(panel_root, core, 1, keepdims=False)
    panel_root, columns, peer, roots_b = lax.optimization_barrier(
        (panel_root, columns, peer, roots_b)
    )
    sums = panel_product(
        jnp.stack([x, z]).astype(jnp.int32),
        jnp.stack(columns),
        panel_root,
        eigen[0] + peer[0] + eigen[1] + peer[1],
    )
    pieces = []
    for half in range(2):
        mine = sums[4 * half : 4 * half + 4]
        pieces.append(
            [mine[0]]
            + [lax.ppermute(mine[s], axes[1 - half], ring(s)) for s in (1, 2, 3)]
        )
    roots_c = find_roots(rank + CUT_B * GROUP, pw, state[:, CUT_B:])

    def added(side):
        return jnp.stack([p[0][side] + p[1][side] + p[2][side] + p[3][side] for p in pieces])

    roots = copies(jnp.concatenate([roots_a, roots_b, roots_c]), ROW)
    got = lax.ppermute(added(1), "core", swap)
    keep = added(0)
    panel = jnp.where(
        core == 0, jnp.concatenate([keep, got], axis=2), jnp.concatenate([got, keep], axis=2)
    )
    return roots.reshape(-1), jnp.moveaxis(panel, 0, 1)


def solution(mesh):
    torus = Mesh(mesh.devices.reshape(4, 4, 4, 2), ALL)
    placed = (P(ROW), P(ROW), P(COL), P(COL), P(), P(None, ROW), P(COL, None, ROW))
    return jax.shard_map(
        merge,
        mesh=torus,
        in_specs=placed,
        out_specs=(P(COL), P(COL + ROW, None, None)),
        check_vma=False,
    )
```

```python
import jax
import jax.numpy as jnp
from jax import lax
from jax.experimental import pallas as pl
from jax.experimental.pallas import tpu as pltpu
from jax.sharding import Mesh
from jax.sharding import PartitionSpec as P

ITERS = 3
ROW = ("z", "x")
COL = ("y", "core")
ALL = ("z", "x", "y", "core")
F32 = jnp.float32
BF16 = jnp.bfloat16
LANES = 128
GROUP = 128
BLOCK = 16
CUT_A = 2


def cost(flops):
    return pl.CostEstimate(flops=int(flops), bytes_accessed=1 << 20, transcendentals=0)


def column(row):
    return jnp.broadcast_to(row, (LANES, LANES)).T


def root_kernel(rank_ref, pw_ref, root_ref, out_ref, w2_ref, ps_ref, c_ref, t_ref, lo_ref, hi_ref):
    w2_ref[...] = pw_ref[1] * pw_ref[1]
    groups = root_ref.shape[1]
    blocks = ps_ref.shape[0] // BLOCK
    for k in range(groups):
        here = pl.ds(k * GROUP, GROUP)
        c_ref[here, :] = column(root_ref[0, k : k + 1, :])
        t_ref[here, :] = column(root_ref[1, k : k + 1, :])
        lo_ref[here, :] = column(root_ref[2, k : k + 1, :])
        hi_ref[here, :] = column(root_ref[3, k : k + 1, :])

    def group_body(g, carry):
        here = pl.ds(g * GROUP, GROUP)
        base = c_ref[pl.ds(g * GROUP + GROUP // 2, 1), :]
        ps_ref[...] = pw_ref[0] - base
        offset = c_ref[here, :] - base
        near_block = jnp.clip((rank_ref[0] // LANES + g - BLOCK // 2) // BLOCK, 0, blocks - 2)

        def step(_, carry):
            t = t_ref[here, :]
            s = offset + t

            def near(r, sums):
                first, second = sums
                for u in range(BLOCK):
                    row = pl.ds((near_block + r) * BLOCK + u, 1)
                    inverse = 1.0 / (ps_ref[row, :] - s)
                    weighted = w2_ref[row, :] * inverse
                    first = first + weighted
                    second = second + weighted * inverse
                return first, second

            def far(i, sums):
                first, second = sums
                for half in range(2):
                    block = 2 * i + half
                    block = jnp.where(block >= near_block, block + 2, block)
                    some = None
                    for u in range(BLOCK):
                        row = pl.ds(block * BLOCK + u, 1)
                        distance = (ps_ref[row, :] - s).astype(BF16)
                        weight = jnp.broadcast_to(w2_ref[row, :], (GROUP, LANES)).astype(BF16)
                        weighted = weight / distance
                        square = weighted / distance
                        some = (weighted, square) if some is None else (some[0] + weighted, some[1] + square)
                    first = first + some[0].astype(F32)
                    second = second + some[1].astype(F32)
                return first, second

            zero = jnp.zeros((GROUP, LANES), F32)
            sums = lax.fori_loop(0, 2, near, (zero, zero))
            first, second = lax.fori_loop(0, (blocks - 2) // 2, far, sums)
            sum_inverse = jnp.sum(first, axis=1, keepdims=True)
            sum_square = jnp.sum(second, axis=1, keepdims=True)
            nearest = jnp.minimum(jnp.abs(lo_ref[here, :] - t), jnp.abs(hi_ref[here, :] - t))
            limit = 0.5 * nearest
            t_ref[here, :] = t - jnp.clip((1.0 + sum_inverse) / sum_square, -limit, limit)
            return carry

        lax.fori_loop(0, ITERS, step, 0)
        return carry

    lax.fori_loop(0, groups, group_body, 0)
    for k in range(groups):
        out_ref[k : k + 1, :] = t_ref[pl.ds(k * GROUP, GROUP), :].T[0:1, :]


def find_roots(rank, pw, root):
    groups = root.shape[1]
    n_pole_rows = pw.shape[1]
    roots = groups * GROUP
    vmem = pl.BlockSpec(memory_space=pltpu.VMEM)
    return pl.pallas_call(
        root_kernel,
        in_specs=[pl.BlockSpec(memory_space=pltpu.SMEM), vmem, vmem],
        out_shape=jax.ShapeDtypeStruct((groups, LANES), F32),
        scratch_shapes=[pltpu.VMEM((n_pole_rows, LANES), F32)] * 2
        + [pltpu.VMEM((roots, LANES), F32)] * 4,
        cost_estimate=cost(ITERS * roots * n_pole_rows * LANES * 10),
        name="find_roots",
    )(rank, pw, root)


def panel_kernel(pw_ref, root_ref, out_ref, w2_ref):
    w2_ref[...] = pw_ref[1] * pw_ref[1]
    count = 16
    c = column(root_ref[0:1, :])[:count]
    t = column(root_ref[1:2, :])[:count]
    unroll = 32
    zero = jnp.zeros((count, LANES), F32)

    def sums_at(t):
        def body(r, sums):
            first, second, nearest = sums
            for u in range(unroll):
                row = pl.ds(r * unroll + u, 1)
                distance = (pw_ref[0, row, :] - c) - t
                inverse = 1.0 / distance
                weighted = w2_ref[row, :] * inverse
                first = first + weighted
                second = second + weighted * inverse
                nearest = jnp.minimum(nearest, jnp.abs(distance))
            return first, second, nearest

        first, second, nearest = lax.fori_loop(
            0, w2_ref.shape[0] // unroll, body, (zero, zero, jnp.full((count, LANES), 3e38, F32))
        )
        return (
            jnp.sum(first, axis=1, keepdims=True),
            jnp.sum(second, axis=1, keepdims=True),
            jnp.min(nearest, axis=1, keepdims=True),
        )

    for _ in range(ITERS):
        sum_inverse, sum_square, nearest = sums_at(t)
        limit = 0.5 * nearest
        t = t - jnp.clip((1.0 + sum_inverse) / sum_square, -limit, limit)
    norm = lax.rsqrt(sums_at(t)[1])
    pad = jnp.zeros((LANES - count, LANES), F32)
    out_ref[0:1, :] = jnp.concatenate([t, pad], axis=0).T[0:1, :]
    out_ref[1:2, :] = jnp.concatenate([jnp.broadcast_to(norm, (count, LANES)), pad], axis=0).T[0:1, :]


def panel_roots(pw, root):
    n_pole_rows = pw.shape[1]
    return pl.pallas_call(
        panel_kernel,
        out_shape=jax.ShapeDtypeStruct((2, LANES), F32),
        scratch_shapes=[pltpu.VMEM((n_pole_rows, LANES), F32)],
        cost_estimate=cost(4 * 20 * n_pole_rows * LANES * 10),
        name="panel_roots",
    )(pw, root)


def pick_kernel(index_ref, pw_ref, out_ref):
    index = jnp.concatenate([index_ref[...], index_ref[...]], axis=0)
    row = index // LANES
    lane = index % LANES
    upper = lax.broadcasted_iota(jnp.int32, (8, LANES), 0) < 4
    unroll = 32

    def body(r, found):
        for u in range(unroll):
            at = r * unroll + u
            values = jnp.where(upper, pw_ref[0, pl.ds(at, 1), :], pw_ref[1, pl.ds(at, 1), :])
            found = jnp.where(row == at, jnp.take_along_axis(values, lane, axis=1), found)
        return found

    out_ref[...] = lax.fori_loop(
        0, pw_ref.shape[1] // unroll, body, jnp.zeros((8, LANES), F32)
    )


def pick_columns(index, pw):
    return pl.pallas_call(
        pick_kernel,
        out_shape=jax.ShapeDtypeStruct((8, LANES), F32),
        cost_estimate=cost(5e7),
        name="pick_columns",
    )(index, pw)


def turn_kernel(place_ref, in_ref, *refs):
    outs = refs[:8]
    wide_ref, half_ref, in_sems, out_sems = refs[8:]
    blocks, rows = wide_ref.shape[:2]

    def fetch(i):
        return pltpu.make_async_copy(in_ref.at[pl.ds(i * rows, rows)], wide_ref.at[i], in_sems.at[i])

    def leave(i, half, shift):
        first = (i % 4 if half == 0 else i // 4) * rows
        return pltpu.make_async_copy(
            half_ref.at[half, i], outs[half * 4 + shift].at[pl.ds(first, rows)], out_sems.at[half, i]
        )

    for i in range(blocks):
        fetch(i).start()

    def body(i, carry):
        fetch(i).wait()
        both = jnp.swapaxes(wide_ref[i], 0, 1)
        for half in range(2):
            half_ref[half, i] = both[half]
            to = ((i // 4 if half == 0 else i % 4) - place_ref[half] + 4) % 4
            for shift in range(4):

                @pl.when(to == shift)
                def _():
                    leave(i, half, shift).start()

        return carry

    lax.fori_loop(0, blocks, body, 0)

    def finish(i, carry):
        for half in range(2):
            leave(i, half, 0).wait()
        return carry

    lax.fori_loop(0, blocks, finish, 0)


def turn_blocks(places, wide):
    n, halves, depth = wide.shape
    rows = n // 16
    hbm = pl.BlockSpec(memory_space=pl.ANY)
    return pl.pallas_call(
        turn_kernel,
        in_specs=[pl.BlockSpec(memory_space=pltpu.SMEM), hbm],
        out_specs=[hbm] * 8,
        out_shape=[jax.ShapeDtypeStruct((n // 4, depth), BF16)] * 8,
        scratch_shapes=[
            pltpu.VMEM((16, rows, halves, depth), BF16),
            pltpu.VMEM((halves, 16, rows, depth), BF16),
            pltpu.SemaphoreType.DMA((16,)),
            pltpu.SemaphoreType.DMA((halves, 16)),
        ],
        cost_estimate=cost(5e7),
        name="turn_blocks",
    )(places, wide)


def matmul_kernel(place_ref, col_ref, root_ref, *refs):
    blocks = refs[:16]
    outs = refs[16:24]
    p_ref, w_ref, e_ref, acc_ref, sems = refs[24:]
    sources = 4
    halves, _, both, depth = e_ref.shape
    rows = both // 2
    quarter = rows // 4
    n_roots = root_ref.shape[1]
    pieces = depth // LANES

    def moves(half, src):
        return [
            pltpu.make_async_copy(
                blocks[half * 8 + side * 4 + src],
                e_ref.at[half, src, pl.ds(side * rows, rows)],
                sems.at[half, src, side],
            )
            for side in range(2)
        ]

    for half in range(halves):
        for src in range(sources):
            for move in moves(half, src):
                move.start()

    def half_body(half, carry):
        for src in range(sources):
            p = jnp.concatenate([col_ref[half, 0, src]] * (LANES // pieces), axis=0).T
            w = jnp.concatenate([col_ref[half, 1, src]] * (LANES // pieces), axis=0).T
            for piece in range(pieces):
                here = pl.ds(src * depth + piece * LANES, LANES)
                p_ref[here, :] = jnp.broadcast_to(p[:, piece : piece + 1], (LANES, LANES))
                w_ref[here, :] = jnp.broadcast_to(w[:, piece : piece + 1], (LANES, LANES))
        for which in range(halves):

            @pl.when(half == which)
            def _():
                for src in range(sources):
                    for move in moves(which, src):
                        move.wait()

        def cauchy(src):
            down = []
            for piece in range(pieces):
                here = pl.ds(src * depth + piece * LANES, LANES)
                p = p_ref[here, :]
                w = w_ref[here, :]
                across = []
                for part in range(n_roots // LANES):
                    lanes = pl.ds(part * LANES, LANES)
                    distance = (p - root_ref[0:1, lanes]) - root_ref[1:2, lanes]
                    value = w * (1.0 / distance) * root_ref[2:3, lanes]
                    across.append(value.astype(BF16))
                down.append(jnp.concatenate(across, axis=1))
            return jnp.concatenate(down, axis=0)

        acc = None
        for src in range(sources):
            product = jnp.dot(e_ref[half, src], cauchy(src), preferred_element_type=F32)
            acc = product if acc is None else acc + product
        acc_ref[...] = acc
        for which in range(halves):

            @pl.when(half == which)
            def _():
                for shift in range(4):
                    part = (place_ref[which] + shift) % 4
                    for side in range(2):
                        piece = acc_ref[pl.ds(side * rows + part * quarter, quarter), :]
                        out = outs[which * 4 + shift]
                        out[side] = piece.astype(out.dtype)

        return carry

    lax.fori_loop(0, halves, half_body, 0)


def panel_product(places, columns, root, blocks):
    rows, depth = blocks[0].shape
    n_roots = root.shape[1]
    shape = (2, rows // 4, n_roots)
    types = [F32, BF16, BF16, BF16] * 2
    vmem = pl.BlockSpec(memory_space=pltpu.VMEM)
    return pl.pallas_call(
        matmul_kernel,
        in_specs=[pl.BlockSpec(memory_space=pltpu.SMEM), vmem, vmem] + [pl.BlockSpec(memory_space=pl.ANY)] * 16,
        out_shape=[jax.ShapeDtypeStruct(shape, t) for t in types],
        scratch_shapes=[pltpu.VMEM((4 * depth, LANES), F32)] * 2
        + [
            pltpu.VMEM((2, 4, 2 * rows, depth), BF16),
            pltpu.VMEM((2 * rows, n_roots), F32),
            pltpu.SemaphoreType.DMA((2, 4, 2)),
        ],
        cost_estimate=cost(2 * 16 * rows * depth * n_roots),
        compiler_params=pltpu.CompilerParams(vmem_limit_bytes=56 << 20),
        name="panel_product",
    )(places, columns, root, *blocks)


def copies(value, axis):
    size = lax.axis_size(axis)
    return lax.all_to_all(
        jnp.broadcast_to(value[None], (size, *value.shape)), axis, 0, 0, tiled=True
    )


def ring(shift):
    return [(i, (i + shift) % 4) for i in range(4)]


def merge(pole_values, weights, centers, offsets, chosen, column_pole, eigen_blocks):
    z = lax.axis_index("z")
    x = lax.axis_index("x")
    core = lax.axis_index("core")
    row = z * 4 + x
    col = lax.axis_index("y") * 2 + core
    n_col = centers.shape[0]
    n_own = n_col // 16
    swap = [(0, 1), (1, 0)]

    parted = jnp.stack([pole_values.reshape(-1, LANES), weights.reshape(-1, LANES)])
    arrived = copies(parted, ROW)

    axes = ("z", "x")
    places = (z, x)
    cut = turn_blocks(jnp.stack(places).astype(jnp.int32), eigen_blocks)

    wanted = lax.dynamic_slice_in_dim(chosen, row * LANES, LANES)
    local = wanted - col * n_col
    hit = local[:, None] == lax.broadcasted_iota(jnp.int32, (1, n_col), 1)
    first = jnp.stack(
        [
            jnp.sum(jnp.where(hit, centers[None, :], 0.0), axis=1),
            jnp.sum(jnp.where(hit, offsets[None, :], 0.0), axis=1),
        ]
    )
    spread = jnp.moveaxis(first.reshape(2, 8, 16), 1, 0)
    arrived, cut, spread = lax.optimization_barrier((arrived, cut, spread))
    cut = (cut[:4], cut[4:])
    pw = jnp.moveaxis(arrived, 1, 0).reshape(2, -1, LANES)
    begun = lax.all_to_all(spread, COL, 0, 0, tiled=True)
    eigen = [[cut[0][0]], [cut[1][0]]]
    for shift in (1, 2, 3):
        for half in range(2):
            eigen[half].append(lax.ppermute(cut[half][shift], axes[half], ring(shift)))
    peer = [[lax.ppermute(eigen[half][0], "core", swap)] for half in range(2)]

    panel_start = jnp.pad(
        jnp.sum(begun, axis=0), ((0, 0), (0, LANES - 16)), constant_values=0.25
    )
    panel_end = panel_roots(pw, panel_start)
    index = lax.dynamic_slice_in_dim(column_pole.reshape(-1, LANES), col * 4, 4)
    picked = pick_columns(index, pw)
    note = jnp.concatenate([picked, panel_start[:1], panel_end], axis=0)
    notes = copies(note, ALL)

    start = col * n_col + row * n_own
    my_centers = lax.dynamic_slice_in_dim(centers.reshape(-1, LANES), row * 4, 4)
    my_offsets = lax.dynamic_slice_in_dim(offsets.reshape(-1, LANES), row * 4, 4)
    own_poles = lax.dynamic_slice_in_dim(pw[0], start // LANES, 4)
    low = own_poles - my_centers
    ranks = start + jnp.arange(n_own).reshape(-1, LANES)
    high = jnp.where(ranks == pw[0].size - 1, 3e38, -low)
    state = jnp.stack([my_centers, my_offsets, low, high])
    rank = start.reshape(1)
    roots_a = find_roots(rank, pw, state[:, :CUT_A])
    eigen, notes, roots_a = lax.optimization_barrier((eigen, notes, roots_a))

    for half in range(2):
        peer[half] += [lax.ppermute(block, "core", swap) for block in eigen[half][1:]]
    roots_b = find_roots(rank + CUT_A * GROUP, pw, state[:, CUT_A:])

    table = notes[:, :8].reshape(4, 4, 2, 4, 2, 4, LANES)
    columns = (
        lax.dynamic_index_in_dim(table[:, :, 0], x, 1, keepdims=False),
        lax.dynamic_index_in_dim(table[:, :, 1], z, 0, keepdims=False),
    )
    columns = [
        jnp.moveaxis(
            jnp.concatenate(
                [lax.dynamic_slice_in_dim(c, (place - s) % 4, 1) for s in range(4)]
            ),
            2,
            0,
        ).reshape(2, 4, -1, LANES)
        for c, place in zip(columns, places)
    ]
    panel_root = jnp.moveaxis(notes[:, 8:, :16], 1, 0).reshape(3, 2, -1)
    panel_root = lax.dynamic_index_in_dim(panel_root, core, 1, keepdims=False)
    panel_root, columns, peer, roots_b = lax.optimization_barrier(
        (panel_root, columns, peer, roots_b)
    )
    roots = copies(jnp.concatenate([roots_a, roots_b]), ROW)
    sums = panel_product(
        jnp.stack([x, z]).astype(jnp.int32),
        jnp.stack(columns),
        panel_root,
        eigen[0] + peer[0] + eigen[1] + peer[1],
    )
    pieces = []
    for half in range(2):
        mine = sums[4 * half : 4 * half + 4]
        pieces.append(
            [mine[0]]
            + [lax.ppermute(mine[s], axes[1 - half], ring(s)) for s in (1, 2, 3)]
        )

    def added(side):
        return jnp.stack([p[0][side] + p[1][side] + p[2][side] + p[3][side] for p in pieces])

    got = lax.ppermute(added(1), "core", swap)
    keep = added(0)
    panel = jnp.where(
        core == 0, jnp.concatenate([keep, got], axis=2), jnp.concatenate([got, keep], axis=2)
    )
    return roots.reshape(-1), jnp.moveaxis(panel, 0, 1)


def solution(mesh):
    torus = Mesh(mesh.devices.reshape(4, 4, 4, 2), ALL)
    placed = (P(ROW), P(ROW), P(COL), P(COL), P(), P(None, ROW), P(COL, None, ROW))
    return jax.shard_map(
        merge,
        mesh=torus,
        in_specs=placed,
        out_specs=(P(COL), P(COL + ROW, None, None)),
        check_vma=False,
    )
```

```python
import jax
import jax.numpy as jnp
from jax import lax
from jax.experimental import pallas as pl
from jax.experimental.pallas import tpu as pltpu
from jax.sharding import Mesh
from jax.sharding import PartitionSpec as P

ITERS = 3
ROW = ("z", "x")
COL = ("y", "core")
ALL = ("z", "x", "y", "core")
F32 = jnp.float32
BF16 = jnp.bfloat16
LANES = 128
GROUP = 128
BLOCK = 16
CUT_A, CUT_B, CUT_C = 1, 2, 3


def cost(flops):
    return pl.CostEstimate(flops=int(flops), bytes_accessed=1 << 20, transcendentals=0)


def column(row):
    return jnp.broadcast_to(row, (LANES, LANES)).T


def root_kernel(rank_ref, pw_ref, root_ref, out_ref, w2_ref, ps_ref, c_ref, t_ref, lo_ref, hi_ref):
    w2_ref[...] = pw_ref[1] * pw_ref[1]
    groups = root_ref.shape[1]
    blocks = ps_ref.shape[0] // BLOCK
    for k in range(groups):
        here = pl.ds(k * GROUP, GROUP)
        c_ref[here, :] = column(root_ref[0, k : k + 1, :])
        t_ref[here, :] = column(root_ref[1, k : k + 1, :])
        lo_ref[here, :] = column(root_ref[2, k : k + 1, :])
        hi_ref[here, :] = column(root_ref[3, k : k + 1, :])

    def group_body(g, carry):
        here = pl.ds(g * GROUP, GROUP)
        base = c_ref[pl.ds(g * GROUP + GROUP // 2, 1), :]
        ps_ref[...] = pw_ref[0] - base
        offset = c_ref[here, :] - base
        near_block = jnp.clip((rank_ref[0] // LANES + g - BLOCK // 2) // BLOCK, 0, blocks - 2)

        def step(_, carry):
            t = t_ref[here, :]
            s = offset + t

            def near(r, sums):
                first, second = sums
                for u in range(BLOCK):
                    row = pl.ds((near_block + r) * BLOCK + u, 1)
                    inverse = 1.0 / (ps_ref[row, :] - s)
                    weighted = w2_ref[row, :] * inverse
                    first = first + weighted
                    second = second + weighted * inverse
                return first, second

            def far(i, sums):
                first, second = sums
                for half in range(2):
                    block = 2 * i + half
                    block = jnp.where(block >= near_block, block + 2, block)
                    some = None
                    for u in range(BLOCK):
                        row = pl.ds(block * BLOCK + u, 1)
                        distance = (ps_ref[row, :] - s).astype(BF16)
                        weight = jnp.broadcast_to(w2_ref[row, :], (GROUP, LANES)).astype(BF16)
                        weighted = weight / distance
                        square = weighted / distance
                        some = (weighted, square) if some is None else (some[0] + weighted, some[1] + square)
                    first = first + some[0].astype(F32)
                    second = second + some[1].astype(F32)
                return first, second

            zero = jnp.zeros((GROUP, LANES), F32)
            sums = lax.fori_loop(0, 2, near, (zero, zero))
            first, second = lax.fori_loop(0, (blocks - 2) // 2, far, sums)
            sum_inverse = jnp.sum(first, axis=1, keepdims=True)
            sum_square = jnp.sum(second, axis=1, keepdims=True)
            nearest = jnp.minimum(jnp.abs(lo_ref[here, :] - t), jnp.abs(hi_ref[here, :] - t))
            limit = 0.5 * nearest
            t_ref[here, :] = t - jnp.clip((1.0 + sum_inverse) / sum_square, -limit, limit)
            return carry

        lax.fori_loop(0, ITERS, step, 0)
        return carry

    lax.fori_loop(0, groups, group_body, 0)
    for k in range(groups):
        out_ref[k : k + 1, :] = t_ref[pl.ds(k * GROUP, GROUP), :].T[0:1, :]


def find_roots(rank, pw, root):
    groups = root.shape[1]
    n_pole_rows = pw.shape[1]
    roots = groups * GROUP
    vmem = pl.BlockSpec(memory_space=pltpu.VMEM)
    return pl.pallas_call(
        root_kernel,
        in_specs=[pl.BlockSpec(memory_space=pltpu.SMEM), vmem, vmem],
        out_shape=jax.ShapeDtypeStruct((groups, LANES), F32),
        scratch_shapes=[pltpu.VMEM((n_pole_rows, LANES), F32)] * 2
        + [pltpu.VMEM((roots, LANES), F32)] * 4,
        cost_estimate=cost(ITERS * roots * n_pole_rows * LANES * 10),
        name="find_roots",
    )(rank, pw, root)


def panel_kernel(pw_ref, root_ref, out_ref, w2_ref):
    w2_ref[...] = pw_ref[1] * pw_ref[1]
    count = 16
    c = column(root_ref[0:1, :])[:count]
    t = column(root_ref[1:2, :])[:count]
    unroll = 32
    zero = jnp.zeros((count, LANES), F32)

    def sums_at(t):
        def body(r, sums):
            first, second, nearest = sums
            for u in range(unroll):
                row = pl.ds(r * unroll + u, 1)
                distance = (pw_ref[0, row, :] - c) - t
                inverse = 1.0 / distance
                weighted = w2_ref[row, :] * inverse
                first = first + weighted
                second = second + weighted * inverse
                nearest = jnp.minimum(nearest, jnp.abs(distance))
            return first, second, nearest

        first, second, nearest = lax.fori_loop(
            0, w2_ref.shape[0] // unroll, body, (zero, zero, jnp.full((count, LANES), 3e38, F32))
        )
        return (
            jnp.sum(first, axis=1, keepdims=True),
            jnp.sum(second, axis=1, keepdims=True),
            jnp.min(nearest, axis=1, keepdims=True),
        )

    for _ in range(ITERS):
        sum_inverse, sum_square, nearest = sums_at(t)
        limit = 0.5 * nearest
        t = t - jnp.clip((1.0 + sum_inverse) / sum_square, -limit, limit)
    norm = lax.rsqrt(sums_at(t)[1])
    pad = jnp.zeros((LANES - count, LANES), F32)
    out_ref[0:1, :] = jnp.concatenate([t, pad], axis=0).T[0:1, :]
    out_ref[1:2, :] = jnp.concatenate([jnp.broadcast_to(norm, (count, LANES)), pad], axis=0).T[0:1, :]


def panel_roots(pw, root):
    n_pole_rows = pw.shape[1]
    return pl.pallas_call(
        panel_kernel,
        out_shape=jax.ShapeDtypeStruct((2, LANES), F32),
        scratch_shapes=[pltpu.VMEM((n_pole_rows, LANES), F32)],
        cost_estimate=cost(4 * 20 * n_pole_rows * LANES * 10),
        name="panel_roots",
    )(pw, root)


def pick_kernel(index_ref, pw_ref, out_ref):
    index = jnp.concatenate([index_ref[...], index_ref[...]], axis=0)
    row = index // LANES
    lane = index % LANES
    upper = lax.broadcasted_iota(jnp.int32, (8, LANES), 0) < 4
    unroll = 32

    def body(r, found):
        for u in range(unroll):
            at = r * unroll + u
            values = jnp.where(upper, pw_ref[0, pl.ds(at, 1), :], pw_ref[1, pl.ds(at, 1), :])
            found = jnp.where(row == at, jnp.take_along_axis(values, lane, axis=1), found)
        return found

    out_ref[...] = lax.fori_loop(
        0, pw_ref.shape[1] // unroll, body, jnp.zeros((8, LANES), F32)
    )


def pick_columns(index, pw):
    return pl.pallas_call(
        pick_kernel,
        out_shape=jax.ShapeDtypeStruct((8, LANES), F32),
        cost_estimate=cost(5e7),
        name="pick_columns",
    )(index, pw)


def turn_kernel(place_ref, in_ref, *refs):
    outs = refs[:8]
    wide_ref, half_ref, in_sems, out_sems = refs[8:]
    blocks, rows = wide_ref.shape[:2]

    def fetch(i):
        return pltpu.make_async_copy(in_ref.at[pl.ds(i * rows, rows)], wide_ref.at[i], in_sems.at[i])

    def leave(i, half, shift):
        first = (i % 4 if half == 0 else i // 4) * rows
        return pltpu.make_async_copy(
            half_ref.at[half, i], outs[half * 4 + shift].at[pl.ds(first, rows)], out_sems.at[half, i]
        )

    for i in range(blocks):
        fetch(i).start()

    def body(i, carry):
        fetch(i).wait()
        both = jnp.swapaxes(wide_ref[i], 0, 1)
        for half in range(2):
            half_ref[half, i] = both[half]
            to = ((i // 4 if half == 0 else i % 4) - place_ref[half] + 4) % 4
            for shift in range(4):

                @pl.when(to == shift)
                def _():
                    leave(i, half, shift).start()

        return carry

    lax.fori_loop(0, blocks, body, 0)

    def finish(i, carry):
        for half in range(2):
            leave(i, half, 0).wait()
        return carry

    lax.fori_loop(0, blocks, finish, 0)


def turn_blocks(places, wide):
    n, halves, depth = wide.shape
    rows = n // 16
    hbm = pl.BlockSpec(memory_space=pl.ANY)
    return pl.pallas_call(
        turn_kernel,
        in_specs=[pl.BlockSpec(memory_space=pltpu.SMEM), hbm],
        out_specs=[hbm] * 8,
        out_shape=[jax.ShapeDtypeStruct((n // 4, depth), BF16)] * 8,
        scratch_shapes=[
            pltpu.VMEM((16, rows, halves, depth), BF16),
            pltpu.VMEM((halves, 16, rows, depth), BF16),
            pltpu.SemaphoreType.DMA((16,)),
            pltpu.SemaphoreType.DMA((halves, 16)),
        ],
        cost_estimate=cost(5e7),
        name="turn_blocks",
    )(places, wide)


def matmul_kernel(place_ref, col_ref, root_ref, *refs):
    blocks = refs[:16]
    outs = refs[16:20]
    p_ref, w_ref, e_ref, acc_ref, sems = refs[20:]
    sources = 4
    halves, _, both, depth = e_ref.shape
    rows = both // 2
    quarter = rows // 4
    n_roots = root_ref.shape[1]
    pieces = depth // LANES

    def moves(half, src):
        return [
            pltpu.make_async_copy(
                blocks[half * 8 + side * 4 + src],
                e_ref.at[half, src, pl.ds(side * rows, rows)],
                sems.at[half, src, side],
            )
            for side in range(2)
        ]

    for half in range(halves):
        for src in range(sources):
            for move in moves(half, src):
                move.start()

    def half_body(half, carry):
        for src in range(sources):
            p = jnp.concatenate([col_ref[half, 0, src]] * (LANES // pieces), axis=0).T
            w = jnp.concatenate([col_ref[half, 1, src]] * (LANES // pieces), axis=0).T
            for piece in range(pieces):
                here = pl.ds(src * depth + piece * LANES, LANES)
                p_ref[here, :] = jnp.broadcast_to(p[:, piece : piece + 1], (LANES, LANES))
                w_ref[here, :] = jnp.broadcast_to(w[:, piece : piece + 1], (LANES, LANES))
        for which in range(halves):

            @pl.when(half == which)
            def _():
                for src in range(sources):
                    for move in moves(which, src):
                        move.wait()

        def cauchy(src):
            down = []
            for piece in range(pieces):
                here = pl.ds(src * depth + piece * LANES, LANES)
                p = p_ref[here, :]
                w = w_ref[here, :]
                across = []
                for part in range(n_roots // LANES):
                    lanes = pl.ds(part * LANES, LANES)
                    distance = (p - root_ref[0:1, lanes]) - root_ref[1:2, lanes]
                    value = w * (1.0 / distance) * root_ref[2:3, lanes]
                    across.append(value.astype(BF16))
                down.append(jnp.concatenate(across, axis=1))
            return jnp.concatenate(down, axis=0)

        acc = None
        for src in range(sources):
            product = jnp.dot(e_ref[half, src], cauchy(src), preferred_element_type=F32)
            acc = product if acc is None else acc + product
        acc_ref[...] = acc
        for which in range(halves):

            @pl.when(half == which)
            def _():
                for side in range(2):
                    mine = pl.ds(side * rows + place_ref[which] * quarter, quarter)
                    outs[which * 2][side] = acc_ref[mine, :]
                    for part in range(4):
                        first = side * rows + part * quarter
                        piece = acc_ref[first : first + quarter, :]
                        outs[which * 2 + 1][part, side] = piece.astype(BF16)

        return carry

    lax.fori_loop(0, halves, half_body, 0)


def panel_product(places, columns, root, blocks):
    rows, depth = blocks[0].shape
    n_roots = root.shape[1]
    shape = (2, rows // 4, n_roots)
    own = jax.ShapeDtypeStruct(shape, F32)
    send = jax.ShapeDtypeStruct((4, *shape), BF16)
    vmem = pl.BlockSpec(memory_space=pltpu.VMEM)
    return pl.pallas_call(
        matmul_kernel,
        in_specs=[pl.BlockSpec(memory_space=pltpu.SMEM), vmem, vmem] + [pl.BlockSpec(memory_space=pl.ANY)] * 16,
        out_shape=[own, send, own, send],
        scratch_shapes=[pltpu.VMEM((4 * depth, LANES), F32)] * 2
        + [
            pltpu.VMEM((2, 4, 2 * rows, depth), BF16),
            pltpu.VMEM((2 * rows, n_roots), F32),
            pltpu.SemaphoreType.DMA((2, 4, 2)),
        ],
        cost_estimate=cost(2 * 16 * rows * depth * n_roots),
        compiler_params=pltpu.CompilerParams(vmem_limit_bytes=56 << 20),
        name="panel_product",
    )(places, columns, root, *blocks)


def copies(value, axis):
    size = lax.axis_size(axis)
    return lax.all_to_all(
        jnp.broadcast_to(value[None], (size, *value.shape)), axis, 0, 0, tiled=True
    )


def ring(shift):
    return [(i, (i + shift) % 4) for i in range(4)]


def merge(pole_values, weights, centers, offsets, chosen, column_pole, eigen_blocks):
    z = lax.axis_index("z")
    x = lax.axis_index("x")
    core = lax.axis_index("core")
    row = z * 4 + x
    col = lax.axis_index("y") * 2 + core
    n_col = centers.shape[0]
    n_own = n_col // 16
    swap = [(0, 1), (1, 0)]

    parted = jnp.stack([pole_values.reshape(-1, LANES), weights.reshape(-1, LANES)])
    arrived = copies(parted, ROW)

    axes = ("z", "x")
    places = (z, x)
    cut = turn_blocks(jnp.stack(places).astype(jnp.int32), eigen_blocks)

    wanted = lax.dynamic_slice_in_dim(chosen, row * LANES, LANES)
    local = wanted - col * n_col
    hit = local[:, None] == lax.broadcasted_iota(jnp.int32, (1, n_col), 1)
    first = jnp.stack(
        [
            jnp.sum(jnp.where(hit, centers[None, :], 0.0), axis=1),
            jnp.sum(jnp.where(hit, offsets[None, :], 0.0), axis=1),
        ]
    )
    spread = jnp.moveaxis(first.reshape(2, 8, 16), 1, 0)
    arrived, cut, spread = lax.optimization_barrier((arrived, cut, spread))
    cut = (cut[:4], cut[4:])
    pw = jnp.moveaxis(arrived, 1, 0).reshape(2, -1, LANES)
    begun = lax.all_to_all(spread, COL, 0, 0, tiled=True)
    eigen = [[cut[0][0]], [cut[1][0]]]
    for shift in (1, 2, 3):
        for half in range(2):
            eigen[half].append(lax.ppermute(cut[half][shift], axes[half], ring(shift)))
    peer = [[lax.ppermute(eigen[half][0], "core", swap)] for half in range(2)]

    panel_start = jnp.pad(
        jnp.sum(begun, axis=0), ((0, 0), (0, LANES - 16)), constant_values=0.25
    )
    panel_end = panel_roots(pw, panel_start)
    index = lax.dynamic_slice_in_dim(column_pole.reshape(-1, LANES), col * 4, 4)
    picked = pick_columns(index, pw)
    note = jnp.concatenate([picked, panel_start[:1], panel_end], axis=0)
    notes = copies(note, ALL)

    start = col * n_col + row * n_own
    my_centers = lax.dynamic_slice_in_dim(centers.reshape(-1, LANES), row * 4, 4)
    my_offsets = lax.dynamic_slice_in_dim(offsets.reshape(-1, LANES), row * 4, 4)
    own_poles = lax.dynamic_slice_in_dim(pw[0], start // LANES, 4)
    low = own_poles - my_centers
    ranks = start + jnp.arange(n_own).reshape(-1, LANES)
    high = jnp.where(ranks == pw[0].size - 1, 3e38, -low)
    state = jnp.stack([my_centers, my_offsets, low, high])
    rank = start.reshape(1)
    roots_a = find_roots(rank, pw, state[:, :CUT_A])
    eigen, notes, roots_a = lax.optimization_barrier((eigen, notes, roots_a))

    for half in range(2):
        peer[half] += [lax.ppermute(block, "core", swap) for block in eigen[half][1:]]
    roots_b = find_roots(rank + CUT_A * GROUP, pw, state[:, CUT_A:CUT_B])

    table = notes[:, :8].reshape(4, 4, 2, 4, 2, 4, LANES)
    columns = (
        lax.dynamic_index_in_dim(table[:, :, 0], x, 1, keepdims=False),
        lax.dynamic_index_in_dim(table[:, :, 1], z, 0, keepdims=False),
    )
    columns = [
        jnp.moveaxis(
            jnp.concatenate(
                [lax.dynamic_slice_in_dim(c, (place - s) % 4, 1) for s in range(4)]
            ),
            2,
            0,
        ).reshape(2, 4, -1, LANES)
        for c, place in zip(columns, places)
    ]
    panel_root = jnp.moveaxis(notes[:, 8:, :16], 1, 0).reshape(3, 2, -1)
    panel_root = lax.dynamic_index_in_dim(panel_root, core, 1, keepdims=False)
    panel_root, columns, peer, roots_b = lax.optimization_barrier(
        (panel_root, columns, peer, roots_b)
    )
    sums = panel_product(
        jnp.stack([x, z]).astype(jnp.int32),
        jnp.stack(columns),
        panel_root,
        eigen[0] + peer[0] + eigen[1] + peer[1],
    )
    others = lax.broadcasted_iota(jnp.int32, (4, 1, 1, 1), 0)
    totals = []
    roots_cd = []
    for half in range(2):
        cuts = (CUT_B, CUT_C, None)[half : half + 2]
        found = lax.all_to_all(sums[2 * half + 1], axes[1 - half], 0, 0, tiled=True)
        part = find_roots(rank + cuts[0] * GROUP, pw, state[:, cuts[0] : cuts[1]])
        found, part, sums = lax.optimization_barrier((found, part, sums))
        roots_cd.append(part)
        far = jnp.where(others == places[1 - half], 0.0, found.astype(F32))
        totals.append(sums[2 * half] + (far[0] + far[1] + far[2] + far[3]))

    def added(side):
        return jnp.stack([total[side] for total in totals])

    roots = copies(jnp.concatenate([roots_a, roots_b, *roots_cd]), ROW)
    got = lax.ppermute(added(1), "core", swap)
    keep = added(0)
    panel = jnp.where(
        core == 0, jnp.concatenate([keep, got], axis=2), jnp.concatenate([got, keep], axis=2)
    )
    return roots.reshape(-1), jnp.moveaxis(panel, 0, 1)


def solution(mesh):
    torus = Mesh(mesh.devices.reshape(4, 4, 4, 2), ALL)
    placed = (P(ROW), P(ROW), P(COL), P(COL), P(), P(None, ROW), P(COL, None, ROW))
    return jax.shard_map(
        merge,
        mesh=torus,
        in_specs=placed,
        out_specs=(P(COL), P(COL + ROW, None, None)),
        check_vma=False,
    )
```

```python
import jax
import jax.numpy as jnp
from jax import lax
from jax.experimental import pallas as pl
from jax.experimental.pallas import tpu as pltpu
from jax.sharding import Mesh
from jax.sharding import PartitionSpec as P

ITERS = 3
ROW = ("z", "x")
COL = ("y", "core")
ALL = ("z", "x", "y", "core")
F32 = jnp.float32
BF16 = jnp.bfloat16
LANES = 128
GROUP = 128
BLOCK = 16
CUT_A, CUT_B = 2, 3


def cost(flops):
    return pl.CostEstimate(flops=int(flops), bytes_accessed=1 << 20, transcendentals=0)


def column(row):
    return jnp.broadcast_to(row, (LANES, LANES)).T


def root_kernel(rank_ref, pw_ref, root_ref, out_ref, w2_ref, ps_ref, c_ref, t_ref, lo_ref, hi_ref):
    w2_ref[...] = pw_ref[1] * pw_ref[1]
    groups = root_ref.shape[1]
    blocks = ps_ref.shape[0] // BLOCK
    for k in range(groups):
        here = pl.ds(k * GROUP, GROUP)
        c_ref[here, :] = column(root_ref[0, k : k + 1, :])
        t_ref[here, :] = column(root_ref[1, k : k + 1, :])
        lo_ref[here, :] = column(root_ref[2, k : k + 1, :])
        hi_ref[here, :] = column(root_ref[3, k : k + 1, :])

    def group_body(g, carry):
        here = pl.ds(g * GROUP, GROUP)
        base = c_ref[pl.ds(g * GROUP + GROUP // 2, 1), :]
        ps_ref[...] = pw_ref[0] - base
        offset = c_ref[here, :] - base
        near_block = jnp.clip((rank_ref[0] // LANES + g - BLOCK // 2) // BLOCK, 0, blocks - 2)

        def step(_, carry):
            t = t_ref[here, :]
            s = offset + t

            def near(r, sums):
                first, second = sums
                for u in range(BLOCK):
                    row = pl.ds((near_block + r) * BLOCK + u, 1)
                    inverse = 1.0 / (ps_ref[row, :] - s)
                    weighted = w2_ref[row, :] * inverse
                    first = first + weighted
                    second = second + weighted * inverse
                return first, second

            def far(i, sums):
                first, second = sums
                for half in range(2):
                    block = 2 * i + half
                    block = jnp.where(block >= near_block, block + 2, block)
                    some = None
                    for u in range(BLOCK):
                        row = pl.ds(block * BLOCK + u, 1)
                        distance = (ps_ref[row, :] - s).astype(BF16)
                        weight = jnp.broadcast_to(w2_ref[row, :], (GROUP, LANES)).astype(BF16)
                        weighted = weight / distance
                        square = weighted / distance
                        some = (weighted, square) if some is None else (some[0] + weighted, some[1] + square)
                    first = first + some[0].astype(F32)
                    second = second + some[1].astype(F32)
                return first, second

            zero = jnp.zeros((GROUP, LANES), F32)
            sums = lax.fori_loop(0, 2, near, (zero, zero))
            first, second = lax.fori_loop(0, (blocks - 2) // 2, far, sums)
            sum_inverse = jnp.sum(first, axis=1, keepdims=True)
            sum_square = jnp.sum(second, axis=1, keepdims=True)
            nearest = jnp.minimum(jnp.abs(lo_ref[here, :] - t), jnp.abs(hi_ref[here, :] - t))
            limit = 0.5 * nearest
            t_ref[here, :] = t - jnp.clip((1.0 + sum_inverse) / sum_square, -limit, limit)
            return carry

        lax.fori_loop(0, ITERS, step, 0)
        return carry

    lax.fori_loop(0, groups, group_body, 0)
    for k in range(groups):
        out_ref[k : k + 1, :] = t_ref[pl.ds(k * GROUP, GROUP), :].T[0:1, :]


def find_roots(rank, pw, root):
    groups = root.shape[1]
    n_pole_rows = pw.shape[1]
    roots = groups * GROUP
    vmem = pl.BlockSpec(memory_space=pltpu.VMEM)
    return pl.pallas_call(
        root_kernel,
        in_specs=[pl.BlockSpec(memory_space=pltpu.SMEM), vmem, vmem],
        out_shape=jax.ShapeDtypeStruct((groups, LANES), F32),
        scratch_shapes=[pltpu.VMEM((n_pole_rows, LANES), F32)] * 2
        + [pltpu.VMEM((roots, LANES), F32)] * 4,
        cost_estimate=cost(ITERS * roots * n_pole_rows * LANES * 10),
        name="find_roots",
    )(rank, pw, root)


def panel_kernel(pw_ref, root_ref, out_ref, w2_ref):
    w2_ref[...] = pw_ref[1] * pw_ref[1]
    count = 16
    c = column(root_ref[0:1, :])[:count]
    t = column(root_ref[1:2, :])[:count]
    unroll = 32
    zero = jnp.zeros((count, LANES), F32)

    def sums_at(t):
        def body(r, sums):
            first, second, nearest = sums
            for u in range(unroll):
                row = pl.ds(r * unroll + u, 1)
                distance = (pw_ref[0, row, :] - c) - t
                inverse = 1.0 / distance
                weighted = w2_ref[row, :] * inverse
                first = first + weighted
                second = second + weighted * inverse
                nearest = jnp.minimum(nearest, jnp.abs(distance))
            return first, second, nearest

        first, second, nearest = lax.fori_loop(
            0, w2_ref.shape[0] // unroll, body, (zero, zero, jnp.full((count, LANES), 3e38, F32))
        )
        return (
            jnp.sum(first, axis=1, keepdims=True),
            jnp.sum(second, axis=1, keepdims=True),
            jnp.min(nearest, axis=1, keepdims=True),
        )

    for _ in range(ITERS):
        sum_inverse, sum_square, nearest = sums_at(t)
        limit = 0.5 * nearest
        t = t - jnp.clip((1.0 + sum_inverse) / sum_square, -limit, limit)
    norm = lax.rsqrt(sums_at(t)[1])
    pad = jnp.zeros((LANES - count, LANES), F32)
    out_ref[0:1, :] = jnp.concatenate([t, pad], axis=0).T[0:1, :]
    out_ref[1:2, :] = jnp.concatenate([jnp.broadcast_to(norm, (count, LANES)), pad], axis=0).T[0:1, :]


def panel_roots(pw, root):
    n_pole_rows = pw.shape[1]
    return pl.pallas_call(
        panel_kernel,
        out_shape=jax.ShapeDtypeStruct((2, LANES), F32),
        scratch_shapes=[pltpu.VMEM((n_pole_rows, LANES), F32)],
        cost_estimate=cost(4 * 20 * n_pole_rows * LANES * 10),
        name="panel_roots",
    )(pw, root)


def pick_kernel(index_ref, pw_ref, out_ref):
    index = jnp.concatenate([index_ref[...], index_ref[...]], axis=0)
    row = index // LANES
    lane = index % LANES
    upper = lax.broadcasted_iota(jnp.int32, (8, LANES), 0) < 4
    unroll = 32

    def body(r, found):
        for u in range(unroll):
            at = r * unroll + u
            values = jnp.where(upper, pw_ref[0, pl.ds(at, 1), :], pw_ref[1, pl.ds(at, 1), :])
            found = jnp.where(row == at, jnp.take_along_axis(values, lane, axis=1), found)
        return found

    out_ref[...] = lax.fori_loop(
        0, pw_ref.shape[1] // unroll, body, jnp.zeros((8, LANES), F32)
    )


def pick_columns(index, pw):
    return pl.pallas_call(
        pick_kernel,
        out_shape=jax.ShapeDtypeStruct((8, LANES), F32),
        cost_estimate=cost(5e7),
        name="pick_columns",
    )(index, pw)


def turn_kernel(place_ref, in_ref, *refs):
    outs = refs[:8]
    wide_ref, half_ref, in_sems, out_sems = refs[8:]
    blocks, rows = wide_ref.shape[:2]

    def fetch(i):
        return pltpu.make_async_copy(in_ref.at[pl.ds(i * rows, rows)], wide_ref.at[i], in_sems.at[i])

    def leave(i, half, shift):
        first = (i % 4 if half == 0 else i // 4) * rows
        return pltpu.make_async_copy(
            half_ref.at[half, i], outs[half * 4 + shift].at[pl.ds(first, rows)], out_sems.at[half, i]
        )

    for i in range(blocks):
        fetch(i).start()

    def body(i, carry):
        fetch(i).wait()
        both = jnp.swapaxes(wide_ref[i], 0, 1)
        for half in range(2):
            half_ref[half, i] = both[half]
            to = ((i // 4 if half == 0 else i % 4) - place_ref[half] + 4) % 4
            for shift in range(4):

                @pl.when(to == shift)
                def _():
                    leave(i, half, shift).start()

        return carry

    lax.fori_loop(0, blocks, body, 0)

    def finish(i, carry):
        for half in range(2):
            leave(i, half, 0).wait()
        return carry

    lax.fori_loop(0, blocks, finish, 0)


def turn_blocks(places, wide):
    n, halves, depth = wide.shape
    rows = n // 16
    hbm = pl.BlockSpec(memory_space=pl.ANY)
    return pl.pallas_call(
        turn_kernel,
        in_specs=[pl.BlockSpec(memory_space=pltpu.SMEM), hbm],
        out_specs=[hbm] * 8,
        out_shape=[jax.ShapeDtypeStruct((n // 4, depth), BF16)] * 8,
        scratch_shapes=[
            pltpu.VMEM((16, rows, halves, depth), BF16),
            pltpu.VMEM((halves, 16, rows, depth), BF16),
            pltpu.SemaphoreType.DMA((16,)),
            pltpu.SemaphoreType.DMA((halves, 16)),
        ],
        cost_estimate=cost(5e7),
        name="turn_blocks",
    )(places, wide)


def matmul_kernel(place_ref, col_ref, root_ref, *refs):
    blocks = refs[:16]
    outs = refs[16:22]
    p_ref, w_ref, e_ref, acc_ref, sems = refs[22:]
    sources = 4
    halves, _, both, depth = e_ref.shape
    rows = both // 2
    quarter = rows // 4
    n_roots = root_ref.shape[1]
    pieces = depth // LANES

    def moves(half, src):
        return [
            pltpu.make_async_copy(
                blocks[half * 8 + side * 4 + src],
                e_ref.at[half, src, pl.ds(side * rows, rows)],
                sems.at[half, src, side],
            )
            for side in range(2)
        ]

    for half in range(halves):
        for src in range(sources):
            for move in moves(half, src):
                move.start()

    def half_body(half, carry):
        for src in range(sources):
            p = jnp.concatenate([col_ref[half, 0, src]] * (LANES // pieces), axis=0).T
            w = jnp.concatenate([col_ref[half, 1, src]] * (LANES // pieces), axis=0).T
            for piece in range(pieces):
                here = pl.ds(src * depth + piece * LANES, LANES)
                p_ref[here, :] = jnp.broadcast_to(p[:, piece : piece + 1], (LANES, LANES))
                w_ref[here, :] = jnp.broadcast_to(w[:, piece : piece + 1], (LANES, LANES))
        for which in range(halves):

            @pl.when(half == which)
            def _():
                for src in range(sources):
                    for move in moves(which, src):
                        move.wait()

        def cauchy(src):
            down = []
            for piece in range(pieces):
                here = pl.ds(src * depth + piece * LANES, LANES)
                p = p_ref[here, :]
                w = w_ref[here, :]
                across = []
                for part in range(n_roots // LANES):
                    lanes = pl.ds(part * LANES, LANES)
                    distance = (p - root_ref[0:1, lanes]) - root_ref[1:2, lanes]
                    value = w * (1.0 / distance) * root_ref[2:3, lanes]
                    across.append(value.astype(BF16))
                down.append(jnp.concatenate(across, axis=1))
            return jnp.concatenate(down, axis=0)

        acc = None
        for src in range(sources):
            product = jnp.dot(e_ref[half, src], cauchy(src), preferred_element_type=F32)
            acc = product if acc is None else acc + product
        acc_ref[...] = acc
        for which in range(halves):

            @pl.when(half == which)
            def _():
                for side in range(2):
                    mine = pl.ds(side * rows + place_ref[which] * quarter, quarter)
                    outs[which * 4][side] = acc_ref[mine, :]
                    if which == 0:
                        for shift in (1, 2, 3):
                            part = (place_ref[which] + shift) % 4
                            there = pl.ds(side * rows + part * quarter, quarter)
                            outs[shift][side] = acc_ref[there, :].astype(BF16)
                    else:
                        for part in range(4):
                            first = side * rows + part * quarter
                            piece = acc_ref[first : first + quarter, :]
                            outs[5][part, side] = piece.astype(BF16)

        return carry

    lax.fori_loop(0, halves, half_body, 0)


def panel_product(places, columns, root, blocks):
    rows, depth = blocks[0].shape
    n_roots = root.shape[1]
    shape = (2, rows // 4, n_roots)
    own = jax.ShapeDtypeStruct(shape, F32)
    send = jax.ShapeDtypeStruct(shape, BF16)
    sends = jax.ShapeDtypeStruct((4, *shape), BF16)
    vmem = pl.BlockSpec(memory_space=pltpu.VMEM)
    return pl.pallas_call(
        matmul_kernel,
        in_specs=[pl.BlockSpec(memory_space=pltpu.SMEM), vmem, vmem] + [pl.BlockSpec(memory_space=pl.ANY)] * 16,
        out_shape=[own, send, send, send, own, sends],
        scratch_shapes=[pltpu.VMEM((4 * depth, LANES), F32)] * 2
        + [
            pltpu.VMEM((2, 4, 2 * rows, depth), BF16),
            pltpu.VMEM((2 * rows, n_roots), F32),
            pltpu.SemaphoreType.DMA((2, 4, 2)),
        ],
        cost_estimate=cost(2 * 16 * rows * depth * n_roots),
        compiler_params=pltpu.CompilerParams(vmem_limit_bytes=56 << 20),
        name="panel_product",
    )(places, columns, root, *blocks)


def copies(value, axis):
    size = lax.axis_size(axis)
    return lax.all_to_all(
        jnp.broadcast_to(value[None], (size, *value.shape)), axis, 0, 0, tiled=True
    )


def ring(shift):
    return [(i, (i + shift) % 4) for i in range(4)]


def merge(pole_values, weights, centers, offsets, chosen, column_pole, eigen_blocks):
    z = lax.axis_index("z")
    x = lax.axis_index("x")
    core = lax.axis_index("core")
    row = z * 4 + x
    col = lax.axis_index("y") * 2 + core
    n_col = centers.shape[0]
    n_own = n_col // 16
    swap = [(0, 1), (1, 0)]

    parted = jnp.stack([pole_values.reshape(-1, LANES), weights.reshape(-1, LANES)])
    arrived = copies(parted, ROW)

    axes = ("z", "x")
    places = (z, x)
    cut = turn_blocks(jnp.stack(places).astype(jnp.int32), eigen_blocks)

    wanted = lax.dynamic_slice_in_dim(chosen, row * LANES, LANES)
    local = wanted - col * n_col
    hit = local[:, None] == lax.broadcasted_iota(jnp.int32, (1, n_col), 1)
    first = jnp.stack(
        [
            jnp.sum(jnp.where(hit, centers[None, :], 0.0), axis=1),
            jnp.sum(jnp.where(hit, offsets[None, :], 0.0), axis=1),
        ]
    )
    spread = jnp.moveaxis(first.reshape(2, 8, 16), 1, 0)
    arrived, cut, spread = lax.optimization_barrier((arrived, cut, spread))
    cut = (cut[:4], cut[4:])
    pw = jnp.moveaxis(arrived, 1, 0).reshape(2, -1, LANES)
    begun = lax.all_to_all(spread, COL, 0, 0, tiled=True)
    eigen = [[cut[0][0]], [cut[1][0]]]
    for shift in (1, 2, 3):
        for half in range(2):
            eigen[half].append(lax.ppermute(cut[half][shift], axes[half], ring(shift)))
    peer = [[lax.ppermute(eigen[half][0], "core", swap)] for half in range(2)]

    panel_start = jnp.pad(
        jnp.sum(begun, axis=0), ((0, 0), (0, LANES - 16)), constant_values=0.25
    )
    panel_end = panel_roots(pw, panel_start)
    index = lax.dynamic_slice_in_dim(column_pole.reshape(-1, LANES), col * 4, 4)
    picked = pick_columns(index, pw)
    note = jnp.concatenate([picked, panel_start[:1], panel_end], axis=0)
    notes = copies(note, ALL)

    start = col * n_col + row * n_own
    my_centers = lax.dynamic_slice_in_dim(centers.reshape(-1, LANES), row * 4, 4)
    my_offsets = lax.dynamic_slice_in_dim(offsets.reshape(-1, LANES), row * 4, 4)
    own_poles = lax.dynamic_slice_in_dim(pw[0], start // LANES, 4)
    low = own_poles - my_centers
    ranks = start + jnp.arange(n_own).reshape(-1, LANES)
    high = jnp.where(ranks == pw[0].size - 1, 3e38, -low)
    state = jnp.stack([my_centers, my_offsets, low, high])
    rank = start.reshape(1)
    roots_a = find_roots(rank, pw, state[:, :CUT_A])
    eigen, notes, roots_a = lax.optimization_barrier((eigen, notes, roots_a))

    for half in range(2):
        peer[half] += [lax.ppermute(block, "core", swap) for block in eigen[half][1:]]
    roots_b = find_roots(rank + CUT_A * GROUP, pw, state[:, CUT_A:CUT_B])

    table = notes[:, :8].reshape(4, 4, 2, 4, 2, 4, LANES)
    columns = (
        lax.dynamic_index_in_dim(table[:, :, 0], x, 1, keepdims=False),
        lax.dynamic_index_in_dim(table[:, :, 1], z, 0, keepdims=False),
    )
    columns = [
        jnp.moveaxis(
            jnp.concatenate(
                [lax.dynamic_slice_in_dim(c, (place - s) % 4, 1) for s in range(4)]
            ),
            2,
            0,
        ).reshape(2, 4, -1, LANES)
        for c, place in zip(columns, places)
    ]
    panel_root = jnp.moveaxis(notes[:, 8:, :16], 1, 0).reshape(3, 2, -1)
    panel_root = lax.dynamic_index_in_dim(panel_root, core, 1, keepdims=False)
    panel_root, columns, peer, roots_b = lax.optimization_barrier(
        (panel_root, columns, peer, roots_b)
    )
    sums = panel_product(
        jnp.stack([x, z]).astype(jnp.int32),
        jnp.stack(columns),
        panel_root,
        eigen[0] + peer[0] + eigen[1] + peer[1],
    )
    found = [lax.ppermute(sums[s], "x", ring(s)) for s in (1, 2, 3)]
    turned = lax.all_to_all(sums[5], "z", 0, 0, tiled=True)
    roots_c = find_roots(rank + CUT_B * GROUP, pw, state[:, CUT_B:])
    others = lax.broadcasted_iota(jnp.int32, (4, 1, 1, 1), 0)
    far = jnp.where(others == z, 0.0, turned.astype(F32))
    totals = [
        sums[0] + found[0] + found[1] + found[2],
        sums[4] + (far[0] + far[1] + far[2] + far[3]),
    ]

    def added(side):
        return jnp.stack([total[side] for total in totals])

    roots = copies(jnp.concatenate([roots_a, roots_b, roots_c]), ROW)
    got = lax.ppermute(added(1), "core", swap)
    keep = added(0)
    panel = jnp.where(
        core == 0, jnp.concatenate([keep, got], axis=2), jnp.concatenate([got, keep], axis=2)
    )
    return roots.reshape(-1), jnp.moveaxis(panel, 0, 1)


def solution(mesh):
    torus = Mesh(mesh.devices.reshape(4, 4, 4, 2), ALL)
    placed = (P(ROW), P(ROW), P(COL), P(COL), P(), P(None, ROW), P(COL, None, ROW))
    return jax.shard_map(
        merge,
        mesh=torus,
        in_specs=placed,
        out_specs=(P(COL), P(COL + ROW, None, None)),
        check_vma=False,
    )
```

```python
import jax
import jax.numpy as jnp
from jax import lax
from jax.experimental import pallas as pl
from jax.experimental.pallas import tpu as pltpu
from jax.sharding import Mesh
from jax.sharding import PartitionSpec as P

ITERS = 3
ROW = ("z", "x")
COL = ("y", "core")
ALL = ("z", "x", "y", "core")
F32 = jnp.float32
BF16 = jnp.bfloat16
LANES = 128
GROUP = 128
BLOCK = 16
CUT_A, CUT_B = 2, 3


def cost(flops):
    return pl.CostEstimate(flops=int(flops), bytes_accessed=1 << 20, transcendentals=0)


def column(row):
    return jnp.broadcast_to(row, (LANES, LANES)).T


def root_kernel(rank_ref, pw_ref, root_ref, out_ref, w2_ref, ps_ref, c_ref, t_ref, lo_ref, hi_ref):
    w2_ref[...] = pw_ref[1] * pw_ref[1]
    groups = root_ref.shape[1]
    blocks = ps_ref.shape[0] // BLOCK
    for k in range(groups):
        here = pl.ds(k * GROUP, GROUP)
        c_ref[here, :] = column(root_ref[0, k : k + 1, :])
        t_ref[here, :] = column(root_ref[1, k : k + 1, :])
        lo_ref[here, :] = column(root_ref[2, k : k + 1, :])
        hi_ref[here, :] = column(root_ref[3, k : k + 1, :])

    def group_body(g, carry):
        here = pl.ds(g * GROUP, GROUP)
        base = c_ref[pl.ds(g * GROUP + GROUP // 2, 1), :]
        ps_ref[...] = pw_ref[0] - base
        offset = c_ref[here, :] - base
        near_block = jnp.clip((rank_ref[0] // LANES + g - BLOCK // 2) // BLOCK, 0, blocks - 2)

        def step(_, carry):
            t = t_ref[here, :]
            s = offset + t

            def near(r, sums):
                first, second = sums
                for u in range(BLOCK):
                    row = pl.ds((near_block + r) * BLOCK + u, 1)
                    inverse = 1.0 / (ps_ref[row, :] - s)
                    weighted = w2_ref[row, :] * inverse
                    first = first + weighted
                    second = second + weighted * inverse
                return first, second

            def far(i, sums):
                first, second = sums
                for third in range(3):
                    block = 3 * i + third
                    block = jnp.where(block >= near_block, block + 2, block)
                    some = None
                    for u in range(BLOCK):
                        row = pl.ds(block * BLOCK + u, 1)
                        distance = (ps_ref[row, :] - s).astype(BF16)
                        weight = jnp.broadcast_to(w2_ref[row, :], (GROUP, LANES)).astype(BF16)
                        weighted = weight / distance
                        square = weighted / distance
                        some = (weighted, square) if some is None else (some[0] + weighted, some[1] + square)
                    first = first + some[0].astype(F32)
                    second = second + some[1].astype(F32)
                return first, second

            zero = jnp.zeros((GROUP, LANES), F32)
            sums = lax.fori_loop(0, 2, near, (zero, zero))
            first, second = lax.fori_loop(0, (blocks - 2) // 3, far, sums)
            sum_inverse = jnp.sum(first, axis=1, keepdims=True)
            sum_square = jnp.sum(second, axis=1, keepdims=True)
            nearest = jnp.minimum(jnp.abs(lo_ref[here, :] - t), jnp.abs(hi_ref[here, :] - t))
            limit = 0.5 * nearest
            t_ref[here, :] = t - jnp.clip((1.0 + sum_inverse) / sum_square, -limit, limit)
            return carry

        lax.fori_loop(0, ITERS, step, 0)
        return carry

    lax.fori_loop(0, groups, group_body, 0)
    for k in range(groups):
        out_ref[k : k + 1, :] = t_ref[pl.ds(k * GROUP, GROUP), :].T[0:1, :]


def find_roots(rank, pw, root):
    groups = root.shape[1]
    n_pole_rows = pw.shape[1]
    roots = groups * GROUP
    vmem = pl.BlockSpec(memory_space=pltpu.VMEM)
    return pl.pallas_call(
        root_kernel,
        in_specs=[pl.BlockSpec(memory_space=pltpu.SMEM), vmem, vmem],
        out_shape=jax.ShapeDtypeStruct((groups, LANES), F32),
        scratch_shapes=[pltpu.VMEM((n_pole_rows, LANES), F32)] * 2
        + [pltpu.VMEM((roots, LANES), F32)] * 4,
        cost_estimate=cost(ITERS * roots * n_pole_rows * LANES * 10),
        name="find_roots",
    )(rank, pw, root)


def panel_kernel(pw_ref, root_ref, out_ref, w2_ref):
    w2_ref[...] = pw_ref[1] * pw_ref[1]
    count = 16
    c = column(root_ref[0:1, :])[:count]
    t = column(root_ref[1:2, :])[:count]
    unroll = 32
    zero = jnp.zeros((count, LANES), F32)

    def sums_at(t):
        def body(r, sums):
            first, second, nearest = sums
            for u in range(unroll):
                row = pl.ds(r * unroll + u, 1)
                distance = (pw_ref[0, row, :] - c) - t
                inverse = 1.0 / distance
                weighted = w2_ref[row, :] * inverse
                first = first + weighted
                second = second + weighted * inverse
                nearest = jnp.minimum(nearest, jnp.abs(distance))
            return first, second, nearest

        first, second, nearest = lax.fori_loop(
            0, w2_ref.shape[0] // unroll, body, (zero, zero, jnp.full((count, LANES), 3e38, F32))
        )
        return (
            jnp.sum(first, axis=1, keepdims=True),
            jnp.sum(second, axis=1, keepdims=True),
            jnp.min(nearest, axis=1, keepdims=True),
        )

    for _ in range(ITERS):
        sum_inverse, sum_square, nearest = sums_at(t)
        limit = 0.5 * nearest
        t = t - jnp.clip((1.0 + sum_inverse) / sum_square, -limit, limit)

    def squares(r, total):
        for u in range(unroll):
            row = pl.ds(r * unroll + u, 1)
            inverse = 1.0 / ((pw_ref[0, row, :] - c) - t)
            total = total + w2_ref[row, :] * inverse * inverse
        return total

    square = lax.fori_loop(0, w2_ref.shape[0] // unroll, squares, zero)
    norm = lax.rsqrt(jnp.sum(square, axis=1, keepdims=True))
    pad = jnp.zeros((LANES - count, LANES), F32)
    out_ref[0:1, :] = jnp.concatenate([t, pad], axis=0).T[0:1, :]
    out_ref[1:2, :] = jnp.concatenate([jnp.broadcast_to(norm, (count, LANES)), pad], axis=0).T[0:1, :]


def panel_roots(pw, root):
    n_pole_rows = pw.shape[1]
    return pl.pallas_call(
        panel_kernel,
        out_shape=jax.ShapeDtypeStruct((2, LANES), F32),
        scratch_shapes=[pltpu.VMEM((n_pole_rows, LANES), F32)],
        cost_estimate=cost(4 * 20 * n_pole_rows * LANES * 10),
        name="panel_roots",
    )(pw, root)


def pick_kernel(index_ref, pw_ref, out_ref):
    index = jnp.concatenate([index_ref[...], index_ref[...]], axis=0)
    row = index // LANES
    lane = index % LANES
    upper = lax.broadcasted_iota(jnp.int32, (8, LANES), 0) < 4
    unroll = 32

    def body(r, found):
        for u in range(unroll):
            at = r * unroll + u
            values = jnp.where(upper, pw_ref[0, pl.ds(at, 1), :], pw_ref[1, pl.ds(at, 1), :])
            found = jnp.where(row == at, jnp.take_along_axis(values, lane, axis=1), found)
        return found

    out_ref[...] = lax.fori_loop(
        0, pw_ref.shape[1] // unroll, body, jnp.zeros((8, LANES), F32)
    )


def pick_columns(index, pw):
    return pl.pallas_call(
        pick_kernel,
        out_shape=jax.ShapeDtypeStruct((8, LANES), F32),
        cost_estimate=cost(5e7),
        name="pick_columns",
    )(index, pw)


def turn_kernel(place_ref, in_ref, *refs):
    outs = refs[:8]
    wide_ref, half_ref, in_sems, out_sems = refs[8:]
    blocks, rows = wide_ref.shape[:2]

    def fetch(i):
        return pltpu.make_async_copy(in_ref.at[pl.ds(i * rows, rows)], wide_ref.at[i], in_sems.at[i])

    def leave(i, half, shift):
        first = (i % 4 if half == 0 else i // 4) * rows
        return pltpu.make_async_copy(
            half_ref.at[half, i], outs[half * 4 + shift].at[pl.ds(first, rows)], out_sems.at[half, i]
        )

    for i in range(blocks):
        fetch(i).start()

    def body(i, carry):
        fetch(i).wait()
        both = jnp.swapaxes(wide_ref[i], 0, 1)
        for half in range(2):
            half_ref[half, i] = both[half]
            to = ((i // 4 if half == 0 else i % 4) - place_ref[half] + 4) % 4
            for shift in range(4):

                @pl.when(to == shift)
                def _():
                    leave(i, half, shift).start()

        return carry

    lax.fori_loop(0, blocks, body, 0)

    def finish(i, carry):
        for half in range(2):
            leave(i, half, 0).wait()
        return carry

    lax.fori_loop(0, blocks, finish, 0)


def turn_blocks(places, wide):
    n, halves, depth = wide.shape
    rows = n // 16
    hbm = pl.BlockSpec(memory_space=pl.ANY)
    return pl.pallas_call(
        turn_kernel,
        in_specs=[pl.BlockSpec(memory_space=pltpu.SMEM), hbm],
        out_specs=[hbm] * 8,
        out_shape=[jax.ShapeDtypeStruct((n // 4, depth), BF16)] * 8,
        scratch_shapes=[
            pltpu.VMEM((16, rows, halves, depth), BF16),
            pltpu.VMEM((halves, 16, rows, depth), BF16),
            pltpu.SemaphoreType.DMA((16,)),
            pltpu.SemaphoreType.DMA((halves, 16)),
        ],
        cost_estimate=cost(5e7),
        name="turn_blocks",
    )(places, wide)


def matmul_kernel(place_ref, col_ref, root_ref, *refs):
    blocks = refs[:16]
    outs = refs[16:22]
    p_ref, w_ref, e_ref, acc_ref, sems = refs[22:]
    sources = 4
    halves, _, both, depth = e_ref.shape
    rows = both // 2
    quarter = rows // 4
    n_roots = root_ref.shape[1]
    pieces = depth // LANES

    def moves(half, src):
        return [
            pltpu.make_async_copy(
                blocks[half * 8 + side * 4 + src],
                e_ref.at[half, src, pl.ds(side * rows, rows)],
                sems.at[half, src, side],
            )
            for side in range(2)
        ]

    for half in range(halves):
        for src in range(sources):
            for move in moves(half, src):
                move.start()

    def half_body(half, carry):
        for src in range(sources):
            p = jnp.concatenate([col_ref[half, 0, src]] * (LANES // pieces), axis=0).T
            w = jnp.concatenate([col_ref[half, 1, src]] * (LANES // pieces), axis=0).T
            for piece in range(pieces):
                here = pl.ds(src * depth + piece * LANES, LANES)
                p_ref[here, :] = jnp.broadcast_to(p[:, piece : piece + 1], (LANES, LANES))
                w_ref[here, :] = jnp.broadcast_to(w[:, piece : piece + 1], (LANES, LANES))
        for which in range(halves):

            @pl.when(half == which)
            def _():
                for src in range(sources):
                    for move in moves(which, src):
                        move.wait()

        def cauchy(src):
            down = []
            for piece in range(pieces):
                here = pl.ds(src * depth + piece * LANES, LANES)
                p = p_ref[here, :]
                w = w_ref[here, :]
                across = []
                for part in range(n_roots // LANES):
                    lanes = pl.ds(part * LANES, LANES)
                    distance = (p - root_ref[0:1, lanes]) - root_ref[1:2, lanes]
                    value = w * (1.0 / distance) * root_ref[2:3, lanes]
                    across.append(value.astype(BF16))
                down.append(jnp.concatenate(across, axis=1))
            return jnp.concatenate(down, axis=0)

        acc = None
        for src in range(sources):
            product = jnp.dot(e_ref[half, src], cauchy(src), preferred_element_type=F32)
            acc = product if acc is None else acc + product
        acc_ref[...] = acc
        for which in range(halves):

            @pl.when(half == which)
            def _():
                for side in range(2):
                    mine = pl.ds(side * rows + place_ref[which] * quarter, quarter)
                    outs[which * 4][side] = acc_ref[mine, :]
                    if which == 0:
                        for shift in (1, 2, 3):
                            part = (place_ref[which] + shift) % 4
                            there = pl.ds(side * rows + part * quarter, quarter)
                            outs[shift][side] = acc_ref[there, :].astype(BF16)
                    else:
                        for part in range(4):
                            first = side * rows + part * quarter
                            piece = acc_ref[first : first + quarter, :]
                            outs[5][part, side] = piece.astype(BF16)

        return carry

    lax.fori_loop(0, halves, half_body, 0)


def panel_product(places, columns, root, blocks):
    rows, depth = blocks[0].shape
    n_roots = root.shape[1]
    shape = (2, rows // 4, n_roots)
    own = jax.ShapeDtypeStruct(shape, F32)
    send = jax.ShapeDtypeStruct(shape, BF16)
    sends = jax.ShapeDtypeStruct((4, *shape), BF16)
    vmem = pl.BlockSpec(memory_space=pltpu.VMEM)
    return pl.pallas_call(
        matmul_kernel,
        in_specs=[pl.BlockSpec(memory_space=pltpu.SMEM), vmem, vmem] + [pl.BlockSpec(memory_space=pl.ANY)] * 16,
        out_shape=[own, send, send, send, own, sends],
        scratch_shapes=[pltpu.VMEM((4 * depth, LANES), F32)] * 2
        + [
            pltpu.VMEM((2, 4, 2 * rows, depth), BF16),
            pltpu.VMEM((2 * rows, n_roots), F32),
            pltpu.SemaphoreType.DMA((2, 4, 2)),
        ],
        cost_estimate=cost(2 * 16 * rows * depth * n_roots),
        compiler_params=pltpu.CompilerParams(vmem_limit_bytes=56 << 20),
        name="panel_product",
    )(places, columns, root, *blocks)


def copies(value, axis):
    size = lax.axis_size(axis)
    return lax.all_to_all(
        jnp.broadcast_to(value[None], (size, *value.shape)), axis, 0, 0, tiled=True
    )


def ring(shift):
    return [(i, (i + shift) % 4) for i in range(4)]


def merge(pole_values, weights, centers, offsets, chosen, column_pole, eigen_blocks):
    z = lax.axis_index("z")
    x = lax.axis_index("x")
    core = lax.axis_index("core")
    row = z * 4 + x
    col = lax.axis_index("y") * 2 + core
    n_col = centers.shape[0]
    n_own = n_col // 16
    swap = [(0, 1), (1, 0)]

    parted = jnp.stack([pole_values.reshape(-1, LANES), weights.reshape(-1, LANES)])
    arrived = copies(parted, ROW)

    axes = ("z", "x")
    places = (z, x)
    cut = turn_blocks(jnp.stack(places).astype(jnp.int32), eigen_blocks)

    wanted = lax.dynamic_slice_in_dim(chosen, row * LANES, LANES)
    local = wanted - col * n_col
    hit = local[:, None] == lax.broadcasted_iota(jnp.int32, (1, n_col), 1)
    first = jnp.stack(
        [
            jnp.sum(jnp.where(hit, centers[None, :], 0.0), axis=1),
            jnp.sum(jnp.where(hit, offsets[None, :], 0.0), axis=1),
        ]
    )
    spread = jnp.moveaxis(first.reshape(2, 8, 16), 1, 0)
    arrived, cut, spread = lax.optimization_barrier((arrived, cut, spread))
    cut = (cut[:4], cut[4:])
    pw = jnp.moveaxis(arrived, 1, 0).reshape(2, -1, LANES)
    begun = lax.all_to_all(spread, COL, 0, 0, tiled=True)
    eigen = [[cut[0][0]], [cut[1][0]]]
    for shift in (1, 2, 3):
        for half in range(2):
            eigen[half].append(lax.ppermute(cut[half][shift], axes[half], ring(shift)))
    peer = [[lax.ppermute(eigen[half][0], "core", swap)] for half in range(2)]

    panel_start = jnp.pad(
        jnp.sum(begun, axis=0), ((0, 0), (0, LANES - 16)), constant_values=0.25
    )
    panel_end = panel_roots(pw, panel_start)
    index = lax.dynamic_slice_in_dim(column_pole.reshape(-1, LANES), col * 4, 4)
    picked = pick_columns(index, pw)
    note = jnp.concatenate([picked, panel_start[:1], panel_end], axis=0)
    notes = copies(note, ALL)

    start = col * n_col + row * n_own
    my_centers = lax.dynamic_slice_in_dim(centers.reshape(-1, LANES), row * 4, 4)
    my_offsets = lax.dynamic_slice_in_dim(offsets.reshape(-1, LANES), row * 4, 4)
    own_poles = lax.dynamic_slice_in_dim(pw[0], start // LANES, 4)
    low = own_poles - my_centers
    ranks = start + jnp.arange(n_own).reshape(-1, LANES)
    high = jnp.where(ranks == pw[0].size - 1, 3e38, -low)
    state = jnp.stack([my_centers, my_offsets, low, high])
    rank = start.reshape(1)
    roots_a = find_roots(rank, pw, state[:, :CUT_A])
    eigen, notes, roots_a = lax.optimization_barrier((eigen, notes, roots_a))

    for half in range(2):
        peer[half] += [lax.ppermute(block, "core", swap) for block in eigen[half][1:]]
    roots_b = find_roots(rank + CUT_A * GROUP, pw, state[:, CUT_A:CUT_B])

    table = notes[:, :8].reshape(4, 4, 2, 4, 2, 4, LANES)
    columns = (
        lax.dynamic_index_in_dim(table[:, :, 0], x, 1, keepdims=False),
        lax.dynamic_index_in_dim(table[:, :, 1], z, 0, keepdims=False),
    )
    columns = [
        jnp.moveaxis(
            jnp.concatenate(
                [lax.dynamic_slice_in_dim(c, (place - s) % 4, 1) for s in range(4)]
            ),
            2,
            0,
        ).reshape(2, 4, -1, LANES)
        for c, place in zip(columns, places)
    ]
    panel_root = jnp.moveaxis(notes[:, 8:, :16], 1, 0).reshape(3, 2, -1)
    panel_root = lax.dynamic_index_in_dim(panel_root, core, 1, keepdims=False)
    panel_root, columns, peer, roots_b = lax.optimization_barrier(
        (panel_root, columns, peer, roots_b)
    )
    sums = panel_product(
        jnp.stack([x, z]).astype(jnp.int32),
        jnp.stack(columns),
        panel_root,
        eigen[0] + peer[0] + eigen[1] + peer[1],
    )
    found = [lax.ppermute(sums[s], "x", ring(s)) for s in (1, 2, 3)]
    turned = lax.all_to_all(sums[5], "z", 0, 0, tiled=True)
    roots_c = find_roots(rank + CUT_B * GROUP, pw, state[:, CUT_B:])
    others = lax.broadcasted_iota(jnp.int32, (4, 1, 1, 1), 0)
    far = jnp.where(others == z, 0.0, turned.astype(F32))
    totals = [
        sums[0] + found[0] + found[1] + found[2],
        sums[4] + (far[0] + far[1] + far[2] + far[3]),
    ]

    def added(side):
        return jnp.stack([total[side] for total in totals])

    roots = copies(jnp.concatenate([roots_a, roots_b, roots_c]), ROW)
    got = lax.ppermute(added(1), "core", swap)
    keep = added(0)
    panel = jnp.where(
        core == 0, jnp.concatenate([keep, got], axis=2), jnp.concatenate([got, keep], axis=2)
    )
    return roots.reshape(-1), jnp.moveaxis(panel, 0, 1)


def solution(mesh):
    torus = Mesh(mesh.devices.reshape(4, 4, 4, 2), ALL)
    placed = (P(ROW), P(ROW), P(COL), P(COL), P(), P(None, ROW), P(COL, None, ROW))
    return jax.shard_map(
        merge,
        mesh=torus,
        in_specs=placed,
        out_specs=(P(COL), P(COL + ROW, None, None)),
        check_vma=False,
    )
```
